128 devices in a mesh: section: 8 (over y, x_hi), vocab: 16 (over z, x_lo, core).
Axes of the slice: x: 4 (x_hi: 2, x_lo: 2; x = x_hi * 2 + x_lo), y: 4, z: 4, core: 2. Of those that a mesh axis runs over, the one named last changes fastest.
Arguments:
- exit_hidden: bfloat16 [3, 256, 8192], P(None, 'vocab', 'section')
- norm_gain: float32 [3, 8192], P(None, 'section'), may hold values from 0.5 to 1.5
- head_weight: bfloat16 [8192, 65536], P(None, ('section', 'vocab'))
- teacher: float32 [256, 65536], P('vocab', 'section'), as said below
Outputs:
- divergence: float32 [3], replicated
- grad_hidden: bfloat16 [3, 256, 8192], P(None, 'vocab', 'section')
- grad_head: bfloat16 [8192, 65536], P(None, ('section', 'vocab'))
The draws below stay inside these ranges and needn't reach their ends.
Inputs may be any that keep to these rules, and one draw needn't show every extreme that they name: Each row of teacher holds log-probabilities: their exponentials sum to one.
All inputs are finite; a program needn't handle non-finite values.
Results may differ from the reference program's by a relative error of at most 0.0086.
Values may be sent and summed in bfloat16 or wider, within the bound.
A program may use at most 128 MiB of HBM per device.

```python
import math
import jax
import jax.numpy as jnp
from jax import lax

D = 8192
VOCAB = 65536
EXITS = 3
TOK = 256


def draw_exit_hidden(key, part):
    shape = (EXITS, TOK, D)
    ramp = 3.0 ** (jnp.arange(D, dtype=jnp.float32) / D)
    col_scale = jnp.exp(jax.random.uniform(jax.random.fold_in(key, 2), (1, 1, D), minval=0.0, maxval=math.log(2.0))) * ramp
    row_scale = jnp.exp(jax.random.uniform(jax.random.fold_in(key, 1), (EXITS, TOK, 1), minval=0.0, maxval=math.log(10.0)))
    values = jax.random.normal(jax.random.fold_in(key, 3), shape) * row_scale * col_scale
    return values.astype(jnp.bfloat16)


def draw_head_weight(key, part):
    scale = 3.0 / math.sqrt(D)
    values = jax.random.normal(jax.random.fold_in(key, 1), (D, VOCAB)) * scale
    return values.astype(jnp.bfloat16)


def draw_teacher(key, part):
    raw = jax.random.normal(jax.random.fold_in(key, 5), (TOK, VOCAB)) * 3.0
    return jax.nn.log_softmax(raw, axis=-1).astype(jnp.float32)


def setup_inputs(seed: int = 0) -> dict:
    splits = jax.random.split(jax.random.key(seed), 5)
    return {
        "exit_hidden": draw_exit_hidden(jax.random.fold_in(splits[4], 71), 0),
        "norm_gain": jnp.clip(1.0 + 0.1 * jax.random.normal(splits[1], (EXITS, D), jnp.float32), 0.5, 1.5),
        "head_weight": draw_head_weight(jax.random.fold_in(splits[4], 71), 0),
        "teacher": draw_teacher(jax.random.fold_in(splits[4], 71), 0),
    }


epsilon = 1e-05
loss_scale = 1024.0

def reference(exit_hidden, norm_gain, head_weight, teacher):
    hidden = exit_hidden.astype(jnp.float32)
    gains = norm_gain.astype(jnp.float32)[:, None, :]
    squares = lax.optimization_barrier(jnp.sum(hidden * hidden, axis=-1, keepdims=True))
    inverse = lax.rsqrt(squares / D + epsilon)
    normed = (hidden * inverse * gains).astype(jnp.bfloat16)
    flat_rows = normed.reshape(EXITS * TOK, D)
    logits = jnp.dot(flat_rows, head_weight, preferred_element_type=jnp.float32).reshape(EXITS, TOK, VOCAB)
    row_max = lax.optimization_barrier(jnp.max(logits, axis=-1))
    log_total = row_max + jnp.log(lax.optimization_barrier(jnp.sum(jnp.exp(logits - row_max[..., None]), axis=-1)))
    target = jnp.exp(teacher)[None]
    cross = lax.optimization_barrier(jnp.sum(target * (teacher[None] - logits), axis=-1))
    weight_sum = lax.optimization_barrier(jnp.sum(target, axis=-1))
    divergence = lax.optimization_barrier(jnp.mean(cross + log_total * weight_sum, axis=-1))
    dlogit = ((jnp.exp(logits - log_total[..., None]) - target) * (loss_scale / TOK)).astype(jnp.bfloat16)
    flat_dlogit = dlogit.reshape(EXITS * TOK, VOCAB)
    grad_head = jnp.dot(flat_rows.T, flat_dlogit, preferred_element_type=jnp.float32).astype(jnp.bfloat16)
    grad_normed = jnp.dot(flat_dlogit, head_weight.T, preferred_element_type=jnp.float32).reshape(EXITS, TOK, D)
    weighted = gains * grad_normed
    inner = lax.optimization_barrier(jnp.sum(weighted * hidden, axis=-1, keepdims=True))
    grad_hidden = (inverse * weighted - hidden * inverse ** 3 * inner / D).astype(jnp.bfloat16)
    return (divergence, grad_hidden, grad_head)
```

```python
import functools

import jax
import jax.numpy as jnp
from jax import lax
from jax.experimental import pallas as pl
from jax.experimental.pallas import tpu as pltpu
from jax.sharding import PartitionSpec as P

MESH = pl.DeviceIdType.MESH
EXITS = 3
ROWS = 16
TOKENS = 256
epsilon = 1e-05
loss_scale = 1024.0
AXES = ("x", "y", "z")
ORDER = (("y", "z", "x"), ("z", "x", "y"), ("x", "y", "z"))
bf16 = jnp.bfloat16
f32 = jnp.float32


def chip(x, y, z, c):
    return (y * 2 + lax.div(x, 2), z * 4 + lax.rem(x, 2) * 2 + c)


def place():
    s, v = lax.axis_index("section"), lax.axis_index("vocab")
    x = lax.rem(s, 2) * 2 + lax.rem(lax.div(v, 2), 2)
    return s, v, dict(x=x, y=lax.div(s, 2), z=lax.div(v, 4)), lax.rem(v, 2)


def turned(k, by):
    return lax.rem(k + by, 4)


class Copies:
    def __init__(self, send_sem, recv_sem):
        self.send_sem, self.recv_sem, self.made = send_sem, recv_sem, []

    def start(self, src, dst, device):
        n = len(self.made)
        copy = pltpu.make_async_remote_copy(
            src_ref=src,
            dst_ref=dst,
            send_sem=self.send_sem.at[n],
            recv_sem=self.recv_sem.at[n],
            device_id=device,
            device_id_type=MESH,
        )
        copy.start()
        self.made.append(copy)
        return copy

    def finish(self):
        for copy in self.made:
            copy.wait_send()


def neighbour(pos, c, axis, by):
    there = dict(pos)
    there[axis] = turned(pos[axis], by)
    return chip(**there, c=c)


def greet(devices):
    barrier = pltpu.get_barrier_semaphore()
    for device in devices:
        pl.semaphore_signal(barrier, inc=1, device_id=device, device_id_type=MESH)
    return lambda: pl.semaphore_wait(barrier, len(devices))


def section_peers(s, v):
    return [(lax.rem(s + k, 8), v) for k in range(1, 8)]


def vocab_peers(s, v):
    return [(s, lax.rem(v + k, 16)) for k in range(1, 16)]


def to_all(copies, slots, me, peers):
    sent = [copies.start(slots.at[me], slots.at[me], peer) for peer in peers]
    for copy in sent:
        copy.wait_recv()


def by_lane(columns, rows):
    lane = lax.broadcasted_iota(jnp.int32, (rows, 128), 1)
    tile = jnp.zeros((rows, 128), f32)
    for k, column in enumerate(columns):
        tile = jnp.where(lane == k, column, tile)
    return tile


def column_of(tile, k):
    lane = lax.broadcasted_iota(jnp.int32, tile.shape, 1)
    return jnp.sum(jnp.where(lane == k, tile, 0.0), axis=1, keepdims=True)


def slots_sum(slots, count):
    total = slots[0]
    for k in range(1, count):
        total = total + slots[k]
    return total


def merged(slots, count):
    top = slots[0]
    for k in range(1, count):
        top = jnp.maximum(top, slots[k])
    exps = jnp.zeros(top.shape, f32)
    sums = jnp.zeros(top.shape, f32)
    for k in range(count):
        part = slots[k]
        exps = exps + jnp.exp(part - top)
        sums = sums + part
    row = lax.broadcasted_iota(jnp.int32, top.shape, 0)
    return jnp.where(row < EXITS, top + jnp.log(exps), sums)


def forward_kernel(
    hidden, gain, teacher, head_hbm, full_hbm, dlogit, divergence, inverse,
    full, head, logits, target, square_slots, vocab_slots, section_slots,
    send_sem, recv_sem, head_sem, full_sem,
):
    width, cols = hidden.shape[2], head.shape[1]
    s, v, pos, c = place()
    x, y, z = pos["x"], pos["y"], pos["z"]
    xh, xl = lax.div(x, 2), lax.rem(x, 2)
    copies = Copies(send_sem, recv_sem)
    head_copy = pltpu.make_async_copy(head_hbm, head, head_sem)
    head_copy.start()
    beyond = neighbour(pos, c, "x", 3 + 2 * xl)
    ready = greet(vocab_peers(s, v) + section_peers(s, v) + [beyond])

    squares = [
        jnp.sum(jnp.square(hidden[e].astype(f32)), axis=1, keepdims=True) for e in range(EXITS)
    ]
    square_slots[s] = by_lane(squares, ROWS)
    ready()
    to_all(copies, square_slots, s, section_peers(s, v))
    inverse[...] = lax.rsqrt(slots_sum(square_slots, 8) / (8 * width) + epsilon)
    for e in range(EXITS):
        scale = column_of(inverse[...], e)
        full[y, xh, e, z, xl, c] = (hidden[e].astype(f32) * scale * gain[e]).astype(bf16)

    half = width // 2

    def region(e, over, whole, part):
        at = {**pos, **over}
        every = slice(None)
        yi, zi = (every if a in whole else at[a] for a in ("y", "z"))
        xhi = every if "x" in whole else lax.div(at["x"], 2)
        xli = every if "x" in whole else lax.rem(at["x"], 2)
        columns = every if part is None else slice(part * half, (part + 1) * half)
        return full.at[yi, xhi, e, zi, xli, c, :, columns]

    partner = chip(**pos, c=1 - c)
    swaps = []

    def swap(ref):
        swaps.append(copies.start(ref, ref, partner))

    for turn in range(3):
        last = turn == 2
        pieces = []
        for e in range(EXITS):
            axis, whole = ORDER[e][turn], ORDER[e][:turn]
            after, before = (neighbour(pos, c, axis, by) for by in (1, 3))
            low, high = region(e, {}, whole, 0), region(e, {}, whole, 1)
            up_low = copies.start(low, low, after)
            down_high = copies.start(high, high, before)
            up_high = copies.start(high, high, after)
            down_low = copies.start(low, low, before)
            pieces.append((up_low, down_high, up_high, down_low))
        if last:
            for e in range(EXITS):
                swap(region(e, {}, ORDER[e][:2], None))
        relays = []
        for e in range(EXITS):
            axis, whole = ORDER[e][turn], ORDER[e][:turn]
            after, before = (neighbour(pos, c, axis, by) for by in (1, 3))
            up_low, down_high, _, _ = pieces[e]
            up_low.wait_recv()
            block = region(e, {axis: turned(pos[axis], 3)}, whole, 0)
            up = copies.start(block, block, after)
            if last:
                swap(block)
            down_high.wait_recv()
            block = region(e, {axis: turned(pos[axis], 1)}, whole, 1)
            down = copies.start(block, block, before)
            if last:
                swap(block)
            relays.append((up, down))
        for e in range(EXITS):
            axis, whole = ORDER[e][turn], ORDER[e][:turn]
            pieces[e][2].wait_recv()
            if last:
                swap(region(e, {axis: turned(pos[axis], 3)}, whole, 1))
            pieces[e][3].wait_recv()
            if last:
                swap(region(e, {axis: turned(pos[axis], 1)}, whole, 0))
        if last:
            lent = [
                copies.start(
                    teacher.at[:, pl.ds(pl.multiple_of(peer[1] * cols, 128), cols)],
                    target.at[v],
                    peer,
                )
                for peer in vocab_peers(s, v)
            ]
            target[v] = teacher[:, pl.ds(pl.multiple_of(v * cols, 128), cols)]
        for e in range(EXITS):
            axis, whole = ORDER[e][turn], ORDER[e][:turn]
            for k in range(2):
                relays[e][k].wait_recv()
                if last:
                    swap(region(e, {axis: turned(pos[axis], 2)}, whole, k))
    for copy in swaps:
        copy.wait_recv()
    full_copy = pltpu.make_async_copy(full, full_hbm, full_sem)
    full_copy.start()
    head_copy.wait()

    logits[...] = jnp.zeros(logits.shape, f32)

    def multiply(k, _):
        rows = full[lax.div(k, 2), lax.rem(k, 2)].reshape(EXITS * TOKENS, width)
        columns = head[pl.ds(pl.multiple_of(k * width, 128), width), :]
        logits[...] += jnp.dot(rows, columns, preferred_element_type=f32)
        return 0

    lax.fori_loop(0, 8, multiply, 0)
    for copy in lent:
        copy.wait_recv()

    columns = []
    for e in range(EXITS):
        block = logits[e * TOKENS : (e + 1) * TOKENS, :]
        top = jnp.max(block, axis=1, keepdims=True)
        columns.append(top + jnp.log(jnp.sum(jnp.exp(block - top), axis=1, keepdims=True)))
    stored = target[...].reshape(TOKENS, cols)
    weight = jnp.exp(stored)
    for e in range(EXITS):
        block = logits[e * TOKENS : (e + 1) * TOKENS, :]
        columns.append(jnp.sum(weight * (stored - block), axis=1, keepdims=True))
    columns.append(jnp.sum(weight, axis=1, keepdims=True))
    vocab_slots[v] = jnp.transpose(by_lane(columns, TOKENS))[:8]
    to_all(copies, vocab_slots, v, vocab_peers(s, v))
    section_slots[s] = merged(vocab_slots, 16)
    to_all(copies, section_slots, s, section_peers(s, v))
    rows = merged(section_slots, 8)
    terms = rows[EXITS : 2 * EXITS] + rows[:EXITS] * rows[2 * EXITS : 2 * EXITS + 1]
    mean = jnp.sum(terms, axis=1, keepdims=True) / TOKENS
    divergence[...] = jnp.broadcast_to(mean, (EXITS, 128))
    turned_rows = jnp.transpose(jnp.concatenate([rows, jnp.zeros((120, TOKENS), f32)], axis=0))
    for e in range(EXITS):
        block = logits[e * TOKENS : (e + 1) * TOKENS, :]
        log_total = turned_rows[:, e : e + 1]
        grad = (jnp.exp(block - log_total) - weight) * (loss_scale / TOKENS)
        dlogit[e * TOKENS : (e + 1) * TOKENS, :] = grad.astype(bf16)
    copies.finish()
    full_copy.wait()


def backward_kernel(
    dlogit, hidden, gain, inverse, head_hbm, grad_hidden,
    head, partial, swapped, held, first, second, third, summed, inner_slots,
    send_sem, recv_sem, swap_send, swap_recv, head_sem,
):
    width = hidden.shape[2]
    s, v, pos, c = place()
    x, y, z = pos["x"], pos["y"], pos["z"]
    copies = Copies(send_sem, recv_sem)

    def head_copy(k):
        rows = pl.ds(pl.multiple_of(k * width, 128), width)
        return pltpu.make_async_copy(head_hbm.at[rows, :], head.at[rows, :], head_sem.at[k])

    for k in range(8):
        head_copy(k).start()
    partner = chip(**pos, c=1 - c)
    near = [neighbour(pos, c, axis, by) for axis in ("x", "z") for by in (1, 3)]
    ready = greet([partner] + section_peers(s, v) + near)
    ready()

    def swap(k):
        yk, xk = lax.div(k, 2), lax.rem(k, 2)
        return pltpu.make_async_remote_copy(
            src_ref=partial.at[yk, xk, :, :, :, 1 - c],
            dst_ref=swapped.at[yk, xk],
            send_sem=swap_send.at[k],
            recv_sem=swap_recv.at[k],
            device_id=partner,
            device_id_type=MESH,
        )

    def multiply(k, _):
        head_copy(k).wait()
        rows = head[pl.ds(pl.multiple_of(k * width, 128), width), :]
        part = lax.dot_general(
            dlogit[...], rows, (((1,), (1,)), ((), ())), preferred_element_type=f32
        )
        partial[lax.div(k, 2), lax.rem(k, 2)] = part.astype(bf16).reshape(EXITS, 4, 2, 2, ROWS, width)
        swap(k).start()
        return 0

    lax.fori_loop(0, 8, multiply, 0)

    def add_swapped(k, _):
        yk, xk = lax.div(k, 2), lax.rem(k, 2)
        swap(k).wait_recv()
        for e in range(EXITS):
            for low in range(2):
                mine = partial[yk, xk, e, :, low, c].astype(f32)
                theirs = swapped[yk, xk, e, :, low].astype(f32)
                held[e, xk * 2 + low, yk] = (mine + theirs).astype(bf16)
        return 0

    lax.fori_loop(0, 8, add_swapped, 0)

    half = width // 2

    def columns_of(part):
        return slice(part * half, (part + 1) * half)

    def block(e, axis, at, rest, part):
        index = [
            slice(None) if a in rest else (at if a == axis else pos[a]) for a in AXES
        ]
        return held.at[(e, *index, slice(None), columns_of(part))]

    def add(e, axis, at, rest, part, arrived):
        def step(n, _):
            digits, index = n, {**pos, axis: at}
            found = []
            for a in reversed(rest):
                found.insert(0, lax.rem(digits, 4))
                index[a] = found[0]
                digits = lax.div(digits, 4)
            ref = held.at[e, index["x"], index["y"], index["z"], :, columns_of(part)]
            total = ref[...].astype(f32)
            for slot in arrived:
                total = total + slot[tuple(found)].astype(f32)
            ref[...] = total.astype(bf16)
            return 0

        lax.fori_loop(0, 4 ** len(rest), step, 0)

    for turn, slots in enumerate((first, second, third)):
        went = []
        plan = []
        for e in range(EXITS):
            axis = ORDER[e][2 - turn]
            rest = tuple(a for a in AXES if a in ORDER[e][: 2 - turn])
            here = pos[axis]
            after, before = (neighbour(pos, c, axis, by) for by in (1, 3))
            plan.append((axis, rest, here, after, before))
            up, down, far = turned(here, 1), turned(here, 3), turned(here, 2)
            went.append(
                [
                    copies.start(block(e, axis, far, rest, 0), slots.at[e, 0], after),
                    copies.start(block(e, axis, far, rest, 1), slots.at[e, 1], before),
                    copies.start(block(e, axis, up, rest, 1), slots.at[e, 3], after),
                    copies.start(block(e, axis, down, rest, 0), slots.at[e, 4], before),
                ]
            )
        for e in range(EXITS):
            axis, rest, here, after, before = plan[e]
            up, down = turned(here, 1), turned(here, 3)
            went[e][0].wait_recv()
            add(e, axis, up, rest, 0, [slots.at[e, 0]])
            went[e].append(copies.start(block(e, axis, up, rest, 0), slots.at[e, 2], after))
            went[e][1].wait_recv()
            add(e, axis, down, rest, 1, [slots.at[e, 1]])
            went[e].append(copies.start(block(e, axis, down, rest, 1), slots.at[e, 5], before))
        for e in range(EXITS):
            axis, rest, here, after, before = plan[e]
            for k in range(2, 6):
                went[e][k].wait_recv()
            if turn < 2:
                add(e, axis, here, rest, 0, [slots.at[e, 2], slots.at[e, 4]])
                add(e, axis, here, rest, 1, [slots.at[e, 3], slots.at[e, 5]])
            else:
                for part in range(2):
                    own = held[e, x, y, z, :, columns_of(part)].astype(f32)
                    near_two = slots[e, 2 + part].astype(f32) + slots[e, 4 + part].astype(f32)
                    summed[e, :, columns_of(part)] = own + near_two

    sums = []
    for e in range(EXITS):
        weighted = gain[e] * summed[e]
        summed[e] = weighted
        sums.append(jnp.sum(weighted * hidden[e].astype(f32), axis=1, keepdims=True))
    inner_slots[s] = by_lane(sums, ROWS)
    to_all(copies, inner_slots, s, section_peers(s, v))
    inner = slots_sum(inner_slots, 8)
    cube = inverse[...] * inverse[...] * inverse[...] * inner / (8 * width)
    for e in range(EXITS):
        scale = column_of(inverse[...], e)
        back = scale * summed[e] - hidden[e].astype(f32) * column_of(cube, e)
        grad_hidden[e] = back.astype(bf16)
    copies.finish()
    for k in range(8):
        swap(k).wait_send()


def body(exit_hidden, norm_gain, head_weight, teacher):
    width, cols = exit_hidden.shape[2], head_weight.shape[1]
    gain = norm_gain[:, None, :]
    vmem = pl.BlockSpec(memory_space=pltpu.VMEM)
    hbm = pl.BlockSpec(memory_space=pl.ANY)
    tile = (4, 2, EXITS, 4, 2, 2, ROWS, width)
    dma = pltpu.SemaphoreType.DMA
    full, dlogit, divergence, inverse = pl.pallas_call(
        forward_kernel,
        out_shape=(
            jax.ShapeDtypeStruct(tile, bf16),
            jax.ShapeDtypeStruct((EXITS * TOKENS, cols), bf16),
            jax.ShapeDtypeStruct((EXITS, 128), f32),
            jax.ShapeDtypeStruct((ROWS, 128), f32),
        ),
        in_specs=[vmem, vmem, vmem, hbm],
        out_specs=(hbm, vmem, vmem, vmem),
        scratch_shapes=[
            pltpu.VMEM(tile, bf16),
            pltpu.VMEM((8 * width, cols), bf16),
            pltpu.VMEM((EXITS * TOKENS, cols), f32),
            pltpu.VMEM((16, ROWS, cols), f32),
            pltpu.VMEM((8, ROWS, 128), f32),
            pltpu.VMEM((16, 8, TOKENS), f32),
            pltpu.VMEM((8, 8, TOKENS), f32),
            dma((119,)),
            dma((119,)),
            dma,
            dma,
        ],
        compiler_params=pltpu.CompilerParams(
            collective_id=0, has_side_effects=True, vmem_limit_bytes=48 * 2**20
        ),
        name="forward",
    )(exit_hidden, gain, teacher, head_weight)
    grad_head = lax.dot_general(
        full.reshape(8, EXITS * TOKENS, width),
        dlogit,
        (((1,), (0,)), ((), ())),
        preferred_element_type=f32,
    ).astype(bf16)
    grad_hidden = pl.pallas_call(
        backward_kernel,
        out_shape=jax.ShapeDtypeStruct(exit_hidden.shape, bf16),
        in_specs=[vmem, vmem, vmem, vmem, hbm],
        out_specs=vmem,
        scratch_shapes=[
            pltpu.VMEM((8 * width, cols), bf16),
            pltpu.VMEM(tile, bf16),
            pltpu.VMEM((4, 2, EXITS, 4, 2, ROWS, width), bf16),
            pltpu.VMEM((EXITS, 4, 4, 4, ROWS, width), bf16),
            pltpu.VMEM((EXITS, 6, 4, 4, ROWS, width // 2), bf16),
            pltpu.VMEM((EXITS, 6, 4, ROWS, width // 2), bf16),
            pltpu.VMEM((EXITS, 6, ROWS, width // 2), bf16),
            pltpu.VMEM((EXITS, ROWS, width), f32),
            pltpu.VMEM((8, ROWS, 128), f32),
            dma((61,)),
            dma((61,)),
            dma((8,)),
            dma((8,)),
            dma((8,)),
        ],
        compiler_params=pltpu.CompilerParams(
            collective_id=1, has_side_effects=True, vmem_limit_bytes=56 * 2**20
        ),
        name="backward",
    )(dlogit, exit_hidden, gain, inverse, head_weight)
    return divergence[:, 0], grad_hidden, grad_head.reshape(8 * width, cols)


def solution(mesh):
    return jax.shard_map(
        body,
        mesh=mesh,
        in_specs=(
            P(None, "vocab", "section"),
            P(None, "section"),
            P(None, ("section", "vocab")),
            P("vocab", "section"),
        ),
        out_specs=(P(), P(None, "vocab", "section"), P(None, ("section", "vocab"))),
        check_vma=False,
    )
```

```python
import functools

import jax
import jax.numpy as jnp
from jax import lax
from jax.experimental import pallas as pl
from jax.experimental.pallas import tpu as pltpu
from jax.sharding import PartitionSpec as P

MESH = pl.DeviceIdType.MESH
EXITS = 3
ROWS = 16
TOKENS = 256
epsilon = 1e-05
loss_scale = 1024.0
AXES = ("x", "y", "z")
ORDER = (("y", "z", "x"), ("z", "x", "y"), ("x", "y", "z"))
bf16 = jnp.bfloat16
f32 = jnp.float32


def chip(x, y, z, c):
    return (y * 2 + lax.div(x, 2), z * 4 + lax.rem(x, 2) * 2 + c)


def place():
    s, v = lax.axis_index("section"), lax.axis_index("vocab")
    x = lax.rem(s, 2) * 2 + lax.rem(lax.div(v, 2), 2)
    return s, v, dict(x=x, y=lax.div(s, 2), z=lax.div(v, 4)), lax.rem(v, 2)


def turned(k, by):
    return lax.rem(k + by, 4)


class Copies:
    def __init__(self, send_sem, recv_sem):
        self.send_sem, self.recv_sem, self.made = send_sem, recv_sem, []

    def start(self, src, dst, device):
        n = len(self.made)
        copy = pltpu.make_async_remote_copy(
            src_ref=src,
            dst_ref=dst,
            send_sem=self.send_sem.at[n],
            recv_sem=self.recv_sem.at[n],
            device_id=device,
            device_id_type=MESH,
        )
        copy.start()
        self.made.append(copy)
        return copy

    def finish(self):
        for copy in self.made:
            copy.wait_send()


def neighbour(pos, c, axis, by):
    there = dict(pos)
    there[axis] = turned(pos[axis], by)
    return chip(**there, c=c)


def greet(devices):
    barrier = pltpu.get_barrier_semaphore()
    for device in devices:
        pl.semaphore_signal(barrier, inc=1, device_id=device, device_id_type=MESH)
    return lambda: pl.semaphore_wait(barrier, len(devices))


def section_peers(s, v):
    return [(lax.rem(s + k, 8), v) for k in range(1, 8)]


def vocab_peers(s, v):
    return [(s, lax.rem(v + k, 16)) for k in range(1, 16)]


DIMS = (("y", 4), ("xh", 2), ("z", 4), ("xl", 2))


def split_x(pos):
    return {
        "y": pos["y"],
        "xh": lax.div(pos["x"], 2),
        "z": pos["z"],
        "xl": lax.rem(pos["x"], 2),
    }


def whole_dims(whole):
    return [(d, n) for d, n in DIMS if d[0] in whole]


def to_all(copies, slots, me, peers):
    sent = [copies.start(slots.at[me], slots.at[me], peer) for peer in peers]
    for copy in sent:
        copy.wait_recv()


def by_lane(columns, rows):
    lane = lax.broadcasted_iota(jnp.int32, (rows, 128), 1)
    tile = jnp.zeros((rows, 128), f32)
    for k, column in enumerate(columns):
        tile = jnp.where(lane == k, column, tile)
    return tile


def column_of(tile, k):
    lane = lax.broadcasted_iota(jnp.int32, tile.shape, 1)
    return jnp.sum(jnp.where(lane == k, tile, 0.0), axis=1, keepdims=True)


def slots_sum(slots, count):
    total = slots[0]
    for k in range(1, count):
        total = total + slots[k]
    return total


def merged(slots, count):
    top = slots[0]
    for k in range(1, count):
        top = jnp.maximum(top, slots[k])
    exps = jnp.zeros(top.shape, f32)
    sums = jnp.zeros(top.shape, f32)
    for k in range(count):
        part = slots[k]
        exps = exps + jnp.exp(part - top)
        sums = sums + part
    row = lax.broadcasted_iota(jnp.int32, top.shape, 0)
    return jnp.where(row < EXITS, top + jnp.log(exps), sums)


def kernel(
    hidden_hbm, gain_hbm, teacher_hbm, head_hbm, divergence, grad_hidden, grad_head,
    hidden, gain, teacher, full, head, logits, target, dlogit, inverse, summed, partial, swapped,
    first_0, first_1, first_2, second_0, second_1, second_2, third,
    square_slots, vocab_slots, section_slots, inner_slots,
    send_sem, recv_sem, swap_send, swap_recv, local_sem,
):
    width, cols = hidden.shape[2], head.shape[1]
    half = width // 2
    s, v, pos, c = place()
    x, y, z = pos["x"], pos["y"], pos["z"]
    xh, xl = lax.div(x, 2), lax.rem(x, 2)
    partner = chip(**pos, c=1 - c)
    copies = Copies(send_sem, recv_sem)
    near = [neighbour(pos, c, "x", by) for by in (1, 3)]
    near += [neighbour(pos, c, "z", by) for by in (1, 2, 3)]
    ready = greet([partner] + section_peers(s, v) + near)
    loads = [
        pltpu.make_async_copy(src, dst, local_sem.at[k])
        for k, (src, dst) in enumerate(
            ((hidden_hbm, hidden), (gain_hbm, gain), (head_hbm, head), (teacher_hbm, teacher))
        )
    ]
    for load in loads:
        load.start()
    loads[0].wait()
    squares = [
        jnp.sum(jnp.square(hidden[e].astype(f32)), axis=1, keepdims=True) for e in range(EXITS)
    ]
    square_slots[s] = by_lane(squares, ROWS)
    loads[1].wait()
    ready()
    to_all(copies, square_slots, s, section_peers(s, v))
    inverse[...] = lax.rsqrt(slots_sum(square_slots, 8) / (8 * width) + epsilon)
    for e in range(EXITS):
        scale = column_of(inverse[...], e)
        normed = hidden[e].astype(f32) * scale * gain[e : e + 1, :]
        full[y, xh, e, z, xl, c] = normed.astype(bf16)

    def columns_of(part):
        return slice(None) if part is None else slice(part * half, (part + 1) * half)

    def region(ref, e, over, whole, part):
        at = split_x({**pos, **over})
        for d, _ in whole_dims(whole):
            at[d] = slice(None)
        return ref.at[at["y"], at["xh"], e, at["z"], at["xl"], c, :, columns_of(part)]

    def around(axis):
        return [neighbour(pos, c, axis, by) for by in (1, 2, 3)]

    swaps = []

    def swap(ref):
        swaps.append(copies.start(ref, ref, partner))

    sent = []
    for e in range(EXITS):
        mine = region(full, e, {}, (), None)
        sent += [copies.start(mine, mine, there) for there in around(ORDER[e][0])]
    for copy in sent:
        copy.wait_recv()
    for turn in (1, 2):
        last = turn == 2
        pieces = []
        for e in range(EXITS):
            axis, whole = ORDER[e][turn], ORDER[e][:turn]
            after, _, before = around(axis)
            low, high = region(full, e, {}, whole, 0), region(full, e, {}, whole, 1)
            up_low = copies.start(low, low, after)
            down_high = copies.start(high, high, before)
            up_high = copies.start(high, high, after)
            down_low = copies.start(low, low, before)
            pieces.append((up_low, down_high, up_high, down_low))
        if last:
            for e in range(EXITS):
                swap(region(full, e, {}, ORDER[e][:2], None))
        relays = []
        for e in range(EXITS):
            axis, whole = ORDER[e][turn], ORDER[e][:turn]
            after, _, before = around(axis)
            up_low, down_high, _, _ = pieces[e]
            up_low.wait_recv()
            block = region(full, e, {axis: turned(pos[axis], 3)}, whole, 0)
            up = copies.start(block, block, after)
            if last:
                swap(block)
            down_high.wait_recv()
            block = region(full, e, {axis: turned(pos[axis], 1)}, whole, 1)
            down = copies.start(block, block, before)
            if last:
                swap(block)
            relays.append((up, down))
        for e in range(EXITS):
            axis, whole = ORDER[e][turn], ORDER[e][:turn]
            pieces[e][2].wait_recv()
            if last:
                swap(region(full, e, {axis: turned(pos[axis], 3)}, whole, 1))
            pieces[e][3].wait_recv()
            if last:
                swap(region(full, e, {axis: turned(pos[axis], 1)}, whole, 0))
        if last:
            loads[3].wait()
            lent = [
                copies.start(
                    teacher.at[:, pl.ds(pl.multiple_of(peer[1] * cols, 128), cols)],
                    target.at[v],
                    peer,
                )
                for peer in vocab_peers(s, v)
            ]
            target[v] = teacher[:, pl.ds(pl.multiple_of(v * cols, 128), cols)]
        for e in range(EXITS):
            axis, whole = ORDER[e][turn], ORDER[e][:turn]
            for k in range(2):
                relays[e][k].wait_recv()
                if last:
                    swap(region(full, e, {axis: turned(pos[axis], 2)}, whole, k))
    for copy in swaps:
        copy.wait_recv()
    loads[2].wait()

    logits[...] = jnp.zeros(logits.shape, f32)

    def rows_of(k):
        return full[lax.div(k, 2), lax.rem(k, 2)].reshape(EXITS * TOKENS, width)

    def head_rows(k):
        return pl.ds(pl.multiple_of(k * width, 128), width)

    def multiply(k, _):
        logits[...] += jnp.dot(rows_of(k), head[head_rows(k), :], preferred_element_type=f32)
        return 0

    lax.fori_loop(0, 8, multiply, 0)
    for copy in lent:
        copy.wait_recv()

    columns = []
    for e in range(EXITS):
        block = logits[e * TOKENS : (e + 1) * TOKENS, :]
        top = jnp.max(block, axis=1, keepdims=True)
        columns.append(top + jnp.log(jnp.sum(jnp.exp(block - top), axis=1, keepdims=True)))
    stored = target[...].reshape(TOKENS, cols)
    weight = jnp.exp(stored)
    for e in range(EXITS):
        block = logits[e * TOKENS : (e + 1) * TOKENS, :]
        columns.append(jnp.sum(weight * (stored - block), axis=1, keepdims=True))
    columns.append(jnp.sum(weight, axis=1, keepdims=True))
    vocab_slots[v] = jnp.transpose(by_lane(columns, TOKENS))[:8]
    to_all(copies, vocab_slots, v, vocab_peers(s, v))
    section_slots[s] = merged(vocab_slots, 16)
    to_all(copies, section_slots, s, section_peers(s, v))
    rows = merged(section_slots, 8)
    turned_rows = jnp.transpose(jnp.concatenate([rows, jnp.zeros((120, TOKENS), f32)], axis=0))
    for e in range(EXITS):
        block = logits[e * TOKENS : (e + 1) * TOKENS, :]
        log_total = turned_rows[:, e : e + 1]
        grad = (jnp.exp(block - log_total) - weight) * (loss_scale / TOKENS)
        dlogit[e * TOKENS : (e + 1) * TOKENS, :] = grad.astype(bf16)

    def exchange(k):
        yk, xk = lax.div(k, 2), lax.rem(k, 2)
        return pltpu.make_async_remote_copy(
            src_ref=partial.at[yk, xk, :, :, :, 1 - c],
            dst_ref=swapped.at[yk, xk],
            send_sem=swap_send.at[k],
            recv_sem=swap_recv.at[k],
            device_id=partner,
            device_id_type=MESH,
        )

    def fold(k, _):
        part = lax.dot_general(
            dlogit[...], head[head_rows(k), :], (((1,), (1,)), ((), ())), preferred_element_type=f32
        )
        shape = (EXITS, 4, 2, 2, ROWS, width)
        partial[lax.div(k, 2), lax.rem(k, 2)] = part.astype(bf16).reshape(shape)
        exchange(k).start()
        return 0

    def add_swapped(k, _):
        yk, xk = lax.div(k, 2), lax.rem(k, 2)
        exchange(k).wait_recv()
        for e in range(EXITS):
            for low in range(2):
                mine = partial[yk, xk, e, :, low, c].astype(f32)
                theirs = swapped[yk, xk, e, :, low].astype(f32)
                partial[yk, xk, e, :, low, c] = (mine + theirs).astype(bf16)
        return 0

    def outer(k, _):
        part = lax.dot_general(
            rows_of(k), dlogit[...], (((0,), (0,)), ((), ())), preferred_element_type=f32
        )
        grad_head[head_rows(k), :] = part.astype(bf16)
        return 0

    lax.fori_loop(0, 8, fold, 0)
    lax.fori_loop(0, 8, add_swapped, 0)
    terms = rows[EXITS : 2 * EXITS] + rows[:EXITS] * rows[2 * EXITS : 2 * EXITS + 1]
    mean = jnp.sum(terms, axis=1, keepdims=True) / TOKENS
    divergence[...] = jnp.broadcast_to(mean, (EXITS, 128))

    def add(e, axis, at, whole, part, arrived):
        dims = whole_dims(whole)

        def step(n, _):
            index = split_x({**pos, axis: at})
            found = []
            for d, size in reversed(dims):
                index[d] = lax.rem(n, size)
                found.insert(0, index[d])
                n = lax.div(n, size)
            ref = partial.at[
                index["y"], index["xh"], e, index["z"], index["xl"], c, :, columns_of(part)
            ]
            total = ref[...].astype(f32)
            for slot in arrived:
                total = total + slot[tuple(found)].astype(f32)
            ref[...] = total.astype(bf16)
            return 0

        lax.fori_loop(0, 4 ** len(whole), step, 0)

    def sums(turn, slots, between):
        went = []
        for e in range(EXITS):
            axis, whole = ORDER[e][2 - turn], ORDER[e][: 2 - turn]
            here = pos[axis]
            after, _, before = around(axis)
            up, far, down = (turned(here, k) for k in (1, 2, 3))
            went.append(
                [
                    copies.start(region(partial, e, {axis: far}, whole, 0), slots[e].at[0], after),
                    copies.start(region(partial, e, {axis: far}, whole, 1), slots[e].at[1], before),
                    copies.start(region(partial, e, {axis: up}, whole, 1), slots[e].at[3], after),
                    copies.start(region(partial, e, {axis: down}, whole, 0), slots[e].at[4], before),
                ]
            )
        between(0)
        for e in range(EXITS):
            axis, whole = ORDER[e][2 - turn], ORDER[e][: 2 - turn]
            here = pos[axis]
            after, _, before = around(axis)
            up, down = turned(here, 1), turned(here, 3)
            went[e][0].wait_recv()
            add(e, axis, up, whole, 0, [slots[e].at[0]])
            block = region(partial, e, {axis: up}, whole, 0)
            went[e].append(copies.start(block, slots[e].at[2], after))
            went[e][1].wait_recv()
            add(e, axis, down, whole, 1, [slots[e].at[1]])
            block = region(partial, e, {axis: down}, whole, 1)
            went[e].append(copies.start(block, slots[e].at[5], before))
        between(1)
        for e in range(EXITS):
            axis, whole = ORDER[e][2 - turn], ORDER[e][: 2 - turn]
            for k in range(2, 6):
                went[e][k].wait_recv()
            for part in range(2):
                add(e, axis, pos[axis], whole, part, [slots[e].at[2 + part], slots[e].at[4 + part]])

    def some_outer(n):
        lax.fori_loop((0, 6)[n], (6, 8)[n], outer, 0)

    sums(0, (first_0, first_1, first_2), some_outer)
    sums(1, (second_0, second_1, second_2), lambda n: None)
    went = []
    for e in range(EXITS):
        axis = ORDER[e][0]
        for k, there in enumerate(around(axis)):
            block = region(partial, e, {axis: turned(pos[axis], k + 1)}, (), None)
            went.append(copies.start(block, third.at[e, k], there))
    inner_sums = []
    for e in range(EXITS):
        total = partial[y, xh, e, z, xl, c].astype(f32)
        for k in range(3):
            went[3 * e + k].wait_recv()
            total = total + third[e, k].astype(f32)
        weighted = gain[e : e + 1, :] * total
        summed[e] = weighted
        inner_sums.append(jnp.sum(weighted * hidden[e].astype(f32), axis=1, keepdims=True))
    inner_slots[s] = by_lane(inner_sums, ROWS)
    to_all(copies, inner_slots, s, section_peers(s, v))
    inner = slots_sum(inner_slots, 8)
    cube = inverse[...] * inverse[...] * inverse[...] * inner / (8 * width)
    for e in range(EXITS):
        scale = column_of(inverse[...], e)
        back = scale * summed[e] - hidden[e].astype(f32) * column_of(cube, e)
        grad_hidden[e] = back.astype(bf16)
    copies.finish()
    for k in range(8):
        exchange(k).wait_send()


def body(exit_hidden, norm_gain, head_weight, teacher):
    width, cols = exit_hidden.shape[2], head_weight.shape[1]
    half = width // 2
    vmem = pl.BlockSpec(memory_space=pltpu.VMEM)
    hbm = pl.BlockSpec(memory_space=pltpu.HBM)
    dma = pltpu.SemaphoreType.DMA
    tile = (4, 2, EXITS, 4, 2, 2, ROWS, width)
    divergence, grad_hidden, grad_head = pl.pallas_call(
        kernel,
        out_shape=(
            jax.ShapeDtypeStruct((EXITS, 128), f32),
            jax.ShapeDtypeStruct(exit_hidden.shape, bf16),
            pltpu.VMEM(head_weight.shape, bf16),
        ),
        in_specs=[hbm] * 4,
        out_specs=(vmem,) * 3,
        scratch_shapes=[
            pltpu.VMEM(exit_hidden.shape, bf16),
            pltpu.VMEM(norm_gain.shape, f32),
            pltpu.VMEM(teacher.shape, f32),
            pltpu.VMEM(tile, bf16),
            pltpu.VMEM(head_weight.shape, bf16),
            pltpu.VMEM((EXITS * TOKENS, cols), f32),
            pltpu.VMEM((16, ROWS, cols), f32),
            pltpu.VMEM((EXITS * TOKENS, cols), bf16),
            pltpu.VMEM((ROWS, 128), f32),
            pltpu.VMEM(exit_hidden.shape, f32),
            pltpu.VMEM(tile, bf16),
            pltpu.VMEM((4, 2, EXITS, 4, 2, ROWS, width), bf16),
        ]
        + [
            pltpu.VMEM((6, *(n for _, n in whole_dims(ORDER[e][:whole])), ROWS, half), bf16)
            for whole in (2, 1)
            for e in range(EXITS)
        ]
        + [
            pltpu.VMEM((EXITS, 3, ROWS, width), bf16),
            pltpu.VMEM((8, ROWS, 128), f32),
            pltpu.VMEM((16, 8, TOKENS), f32),
            pltpu.VMEM((8, 8, TOKENS), f32),
            pltpu.VMEM((8, ROWS, 128), f32),
            dma((162,)),
            dma((162,)),
            dma((8,)),
            dma((8,)),
            dma((4,)),
        ],
        compiler_params=pltpu.CompilerParams(
            collective_id=0, has_side_effects=True, vmem_limit_bytes=53 * 2**20
        ),
        name="exits",
    )(exit_hidden, norm_gain, teacher, head_weight)
    return divergence[:, 0], grad_hidden, grad_head


def solution(mesh):
    return jax.shard_map(
        body,
        mesh=mesh,
        in_specs=(
            P(None, "vocab", "section"),
            P(None, "section"),
            P(None, ("section", "vocab")),
            P("vocab", "section"),
        ),
        out_specs=(P(), P(None, "vocab", "section"), P(None, ("section", "vocab"))),
        check_vma=False,
    )
```

```python
import functools

import jax
import jax.numpy as jnp
from jax import lax
from jax.experimental import pallas as pl
from jax.experimental.pallas import tpu as pltpu
from jax.sharding import PartitionSpec as P

MESH = pl.DeviceIdType.MESH
EXITS = 3
ROWS = 16
TOKENS = 256
epsilon = 1e-05
loss_scale = 1024.0
AXES = ("x", "y", "z")
ORDER = (("y", "z", "x"), ("z", "x", "y"), ("x", "y", "z"))
bf16 = jnp.bfloat16
f32 = jnp.float32


def chip(x, y, z, c):
    return (y * 2 + lax.div(x, 2), z * 4 + lax.rem(x, 2) * 2 + c)


def place():
    s, v = lax.axis_index("section"), lax.axis_index("vocab")
    x = lax.rem(s, 2) * 2 + lax.rem(lax.div(v, 2), 2)
    return s, v, dict(x=x, y=lax.div(s, 2), z=lax.div(v, 4)), lax.rem(v, 2)


def turned(k, by):
    return lax.rem(k + by, 4)


class Copies:
    def __init__(self, send_sem, recv_sem):
        self.send_sem, self.recv_sem, self.made = send_sem, recv_sem, []

    def start(self, src, dst, device):
        n = len(self.made)
        copy = pltpu.make_async_remote_copy(
            src_ref=src,
            dst_ref=dst,
            send_sem=self.send_sem.at[n],
            recv_sem=self.recv_sem.at[n],
            device_id=device,
            device_id_type=MESH,
        )
        copy.start()
        self.made.append(copy)
        return copy

    def finish(self):
        for copy in self.made:
            copy.wait_send()


def neighbour(pos, c, axis, by):
    there = dict(pos)
    there[axis] = turned(pos[axis], by)
    return chip(**there, c=c)


def greet(devices):
    barrier = pltpu.get_barrier_semaphore()
    for device in devices:
        pl.semaphore_signal(barrier, inc=1, device_id=device, device_id_type=MESH)
    return lambda: pl.semaphore_wait(barrier, len(devices))


def section_peers(s, v):
    return [(lax.rem(s + k, 8), v) for k in range(1, 8)]


def vocab_peers(s, v):
    return [(s, lax.rem(v + k, 16)) for k in range(1, 16)]


DIMS = (("y", 4), ("xh", 2), ("z", 4), ("xl", 2))


def split_x(pos):
    return {
        "y": pos["y"],
        "xh": lax.div(pos["x"], 2),
        "z": pos["z"],
        "xl": lax.rem(pos["x"], 2),
    }


def whole_dims(whole):
    return [(d, n) for d, n in DIMS if d[0] in whole]


def to_all(copies, slots, me, peers):
    sent = [copies.start(slots.at[me], slots.at[me], peer) for peer in peers]
    for copy in sent:
        copy.wait_recv()


def by_lane(columns, rows):
    lane = lax.broadcasted_iota(jnp.int32, (rows, 128), 1)
    tile = jnp.zeros((rows, 128), f32)
    for k, column in enumerate(columns):
        tile = jnp.where(lane == k, column, tile)
    return tile


def column_of(tile, k):
    lane = lax.broadcasted_iota(jnp.int32, tile.shape, 1)
    return jnp.sum(jnp.where(lane == k, tile, 0.0), axis=1, keepdims=True)


def slots_sum(slots, count):
    total = slots[0]
    for k in range(1, count):
        total = total + slots[k]
    return total


def merged(slots, count):
    top = slots[0]
    for k in range(1, count):
        top = jnp.maximum(top, slots[k])
    exps = jnp.zeros(top.shape, f32)
    sums = jnp.zeros(top.shape, f32)
    for k in range(count):
        part = slots[k]
        exps = exps + jnp.exp(part - top)
        sums = sums + part
    row = lax.broadcasted_iota(jnp.int32, top.shape, 0)
    return jnp.where(row < EXITS, top + jnp.log(exps), sums)


def kernel(
    hidden_hbm, gain_hbm, teacher_hbm, head_hbm, divergence, grad_hidden, grad_head,
    hidden, gain, teacher, full, head, logits, target, dlogit, inverse, summed, partial, swapped,
    first_0, first_1, first_2, second_0, second_1, second_2, third,
    square_slots, vocab_slots, section_slots, inner_slots,
    send_sem, recv_sem, swap_send, swap_recv, local_sem,
):
    width, cols = hidden.shape[2], head.shape[1]
    half = width // 2
    s, v, pos, c = place()
    x, y, z = pos["x"], pos["y"], pos["z"]
    xh, xl = lax.div(x, 2), lax.rem(x, 2)
    partner = chip(**pos, c=1 - c)
    copies = Copies(send_sem, recv_sem)
    near = [neighbour(pos, c, "x", by) for by in (1, 3)]
    near += [neighbour(pos, c, "z", by) for by in (1, 2, 3)]
    ready = greet([partner] + section_peers(s, v) + near)
    loads = [
        pltpu.make_async_copy(src, dst, local_sem.at[k])
        for k, (src, dst) in enumerate(
            ((hidden_hbm, hidden), (gain_hbm, gain), (head_hbm, head), (teacher_hbm, teacher))
        )
    ]
    for load in loads:
        load.start()
    loads[0].wait()
    squares = [
        jnp.sum(jnp.square(hidden[e].astype(f32)), axis=1, keepdims=True) for e in range(EXITS)
    ]
    square_slots[s] = by_lane(squares, ROWS)
    loads[1].wait()
    ready()
    to_all(copies, square_slots, s, section_peers(s, v))
    inverse[...] = lax.rsqrt(slots_sum(square_slots, 8) / (8 * width) + epsilon)
    for e in range(EXITS):
        scale = column_of(inverse[...], e)
        normed = hidden[e].astype(f32) * scale * gain[e : e + 1, :]
        full[y, xh, e, z, xl, c] = normed.astype(bf16)

    def columns_of(part):
        return slice(None) if part is None else slice(part * half, (part + 1) * half)

    def region(ref, e, over, whole, part):
        at = split_x({**pos, **over})
        for d, _ in whole_dims(whole):
            at[d] = slice(None)
        return ref.at[at["y"], at["xh"], e, at["z"], at["xl"], c, :, columns_of(part)]

    def around(axis):
        return [neighbour(pos, c, axis, by) for by in (1, 2, 3)]

    def swap(ref):
        return copies.start(ref, ref, partner)

    def rows_of(k):
        return full[lax.div(k, 2), lax.rem(k, 2)].reshape(EXITS * TOKENS, width)

    def head_rows(k):
        return pl.ds(pl.multiple_of(k * width, 128), width)

    def across_x(by):
        there = turned(x, by)
        high, low = lax.div(there, 2), lax.rem(there, 2)

        def step(k, _):
            tokens = full[k, high, 0, :, low].reshape(TOKENS // 2, width)
            part = jnp.dot(tokens, head[head_rows(2 * k + high), :], preferred_element_type=f32)
            logits[0, :, low] += part.reshape(4, 2, ROWS, cols)
            return 0

        lax.fori_loop(0, 4, step, 0)

    def across_y(by):
        there = turned(y, by)

        def step(k, _):
            tokens = full[there, k, 1].reshape(TOKENS, width)
            part = jnp.dot(tokens, head[head_rows(2 * there + k), :], preferred_element_type=f32)
            logits[1] += part.reshape(4, 2, 2, ROWS, cols)
            return 0

        lax.fori_loop(0, 2, step, 0)

    def last_exit(k, _):
        tokens = full[lax.div(k, 2), lax.rem(k, 2), 2].reshape(TOKENS, width)
        part = jnp.dot(tokens, head[head_rows(k), :], preferred_element_type=f32)
        logits[2] += part.reshape(4, 2, 2, ROWS, cols)
        return 0

    logits[...] = jnp.zeros(logits.shape, f32)

    sent = []
    for e in range(EXITS):
        mine = region(full, e, {}, (), None)
        sent += [copies.start(mine, mine, there) for there in around(ORDER[e][0])]
    for copy in sent:
        copy.wait_recv()
    for turn in (1, 2):
        last = turn == 2
        pieces = []
        for e in range(EXITS):
            axis, whole = ORDER[e][turn], ORDER[e][:turn]
            after, _, before = around(axis)
            low, high = region(full, e, {}, whole, 0), region(full, e, {}, whole, 1)
            up_low = copies.start(low, low, after)
            down_high = copies.start(high, high, before)
            up_high = copies.start(high, high, after)
            down_low = copies.start(low, low, before)
            pieces.append((up_low, down_high, up_high, down_low))
        if last:
            own_swaps = [swap(region(full, e, {}, ORDER[e][:2], None)) for e in range(EXITS)]
            near_swaps = [[], [], []]
            far_swaps = [[], [], [own_swaps[2]]]
            loads[2].wait()
            for e in range(2):
                own_swaps[e].wait_recv()
                (across_x, across_y)[e](0)
        relays = []
        for e in range(EXITS):
            axis, whole = ORDER[e][turn], ORDER[e][:turn]
            after, _, before = around(axis)
            up_low, down_high, _, _ = pieces[e]
            up_low.wait_recv()
            block = region(full, e, {axis: turned(pos[axis], 3)}, whole, 0)
            up = copies.start(block, block, after)
            if last:
                near_swaps[e].append(swap(block))
            down_high.wait_recv()
            block = region(full, e, {axis: turned(pos[axis], 1)}, whole, 1)
            down = copies.start(block, block, before)
            if last:
                near_swaps[e].append(swap(block))
            relays.append((up, down))
        for e in range(EXITS):
            axis, whole = ORDER[e][turn], ORDER[e][:turn]
            pieces[e][2].wait_recv()
            if last:
                near_swaps[e].append(swap(region(full, e, {axis: turned(pos[axis], 3)}, whole, 1)))
            pieces[e][3].wait_recv()
            if last:
                near_swaps[e].append(swap(region(full, e, {axis: turned(pos[axis], 1)}, whole, 0)))
        if last:
            loads[3].wait()
            lent = [
                copies.start(
                    teacher.at[:, pl.ds(pl.multiple_of(peer[1] * cols, 128), cols)],
                    target.at[v],
                    peer,
                )
                for peer in vocab_peers(s, v)
            ]
            target[v] = teacher[:, pl.ds(pl.multiple_of(v * cols, 128), cols)]
            for e in range(2):
                for copy in near_swaps[e]:
                    copy.wait_recv()
                (across_x, across_y)[e](1)
                (across_x, across_y)[e](3)
            far_swaps[2] += near_swaps[2]
        for e in range(EXITS):
            axis, whole = ORDER[e][turn], ORDER[e][:turn]
            for k in range(2):
                relays[e][k].wait_recv()
                if last:
                    block = region(full, e, {axis: turned(pos[axis], 2)}, whole, k)
                    far_swaps[e].append(swap(block))
    for e in range(EXITS):
        axis, whole = ORDER[e][2], ORDER[e][:2]
        for copy in far_swaps[e]:
            copy.wait_recv()
        if e < 2:
            (across_x, across_y)[e](2)
    lax.fori_loop(0, 8, last_exit, 0)
    for copy in lent:
        copy.wait_recv()

    columns = []
    for e in range(EXITS):
        block = logits[e].reshape(TOKENS, cols)
        top = jnp.max(block, axis=1, keepdims=True)
        columns.append(top + jnp.log(jnp.sum(jnp.exp(block - top), axis=1, keepdims=True)))
    stored = target[...].reshape(TOKENS, cols)
    weight = jnp.exp(stored)
    for e in range(EXITS):
        block = logits[e].reshape(TOKENS, cols)
        columns.append(jnp.sum(weight * (stored - block), axis=1, keepdims=True))
    columns.append(jnp.sum(weight, axis=1, keepdims=True))
    vocab_slots[v] = jnp.transpose(by_lane(columns, TOKENS))[:8]
    to_all(copies, vocab_slots, v, vocab_peers(s, v))
    section_slots[s] = merged(vocab_slots, 16)
    to_all(copies, section_slots, s, section_peers(s, v))
    rows = merged(section_slots, 8)
    turned_rows = jnp.transpose(jnp.concatenate([rows, jnp.zeros((120, TOKENS), f32)], axis=0))
    for e in range(EXITS):
        block = logits[e].reshape(TOKENS, cols)
        log_total = turned_rows[:, e : e + 1]
        grad = (jnp.exp(block - log_total) - weight) * (loss_scale / TOKENS)
        dlogit[e * TOKENS : (e + 1) * TOKENS, :] = grad.astype(bf16)

    def fold_place(k):
        return lax.rem(y + lax.rem(k, 4), 4), lax.rem(xh + 1 - lax.div(k, 4), 2)

    def exchange(k):
        yk, xk = fold_place(k)
        return pltpu.make_async_remote_copy(
            src_ref=partial.at[yk, xk, :, :, :, 1 - c],
            dst_ref=swapped.at[yk, xk],
            send_sem=swap_send.at[k],
            recv_sem=swap_recv.at[k],
            device_id=partner,
            device_id_type=MESH,
        )

    def fold(k, _):
        yk, xk = fold_place(k)
        rows = head[head_rows(2 * yk + xk), :]
        part = lax.dot_general(
            dlogit[...], rows, (((1,), (1,)), ((), ())), preferred_element_type=f32
        )
        shape = (EXITS, 4, 2, 2, ROWS, width)
        partial[yk, xk] = part.astype(bf16).reshape(shape)
        exchange(k).start()
        return 0

    def add_swapped(k, _):
        yk, xk = fold_place(k)
        exchange(k).wait_recv()
        for e in range(EXITS):
            for low in range(2):
                mine = partial[yk, xk, e, :, low, c].astype(f32)
                theirs = swapped[yk, xk, e, :, low].astype(f32)
                partial[yk, xk, e, :, low, c] = (mine + theirs).astype(bf16)
        return 0

    def outer(k, _):
        part = lax.dot_general(
            rows_of(k), dlogit[...], (((0,), (0,)), ((), ())), preferred_element_type=f32
        )
        grad_head[head_rows(k), :] = part.astype(bf16)
        return 0

    terms = rows[EXITS : 2 * EXITS] + rows[:EXITS] * rows[2 * EXITS : 2 * EXITS + 1]
    mean = jnp.sum(terms, axis=1, keepdims=True) / TOKENS
    divergence[...] = jnp.broadcast_to(mean, (EXITS, 128))

    def add(e, axis, at, whole, part, arrived):
        dims = whole_dims(whole)

        def step(n, _):
            index = split_x({**pos, axis: at})
            found = []
            for d, size in reversed(dims):
                index[d] = lax.rem(n, size)
                found.insert(0, index[d])
                n = lax.div(n, size)
            ref = partial.at[
                index["y"], index["xh"], e, index["z"], index["xl"], c, :, columns_of(part)
            ]
            total = ref[...].astype(f32)
            for slot in arrived:
                total = total + slot[tuple(found)].astype(f32)
            ref[...] = total.astype(bf16)
            return 0

        lax.fori_loop(0, 4 ** len(whole), step, 0)

    def first_copies(e, axis, whole, slots):
        after, _, before = around(axis)
        up, far, down = (turned(pos[axis], k) for k in (1, 2, 3))
        return [
            copies.start(region(partial, e, {axis: far}, whole, 0), slots.at[0], after),
            copies.start(region(partial, e, {axis: far}, whole, 1), slots.at[1], before),
            copies.start(region(partial, e, {axis: up}, whole, 1), slots.at[3], after),
            copies.start(region(partial, e, {axis: down}, whole, 0), slots.at[4], before),
        ]

    def first_group(group):
        high = lax.rem(xh + 1 - group, 2)
        went = [[], [], []]
        if group == 0:
            after, _, before = around("x")
            for part, there in ((0, after), (1, before)):
                block = region(partial, 0, {"x": turned(x, 2)}, ("y", "z"), part)
                went[0].append(copies.start(block, first_0.at[part], there))
        side = xl if group == 0 else 1 - xl
        by = 3 + 2 * side
        block = partial.at[
            :, high, 0, :, 1 - xl, c, :, pl.ds(pl.multiple_of(side * half, 128), half)
        ]
        went[0].append(copies.start(block, first_0.at[4 - side], neighbour(pos, c, "x", by)))
        for e, axis, slots in ((1, "y", first_1), (2, "z", first_2)):
            after, _, before = around(axis)
            up, far, down = (turned(pos[axis], k) for k in (1, 2, 3))
            plan = ((far, 0, 0, after), (far, 1, 1, before), (up, 1, 3, after), (down, 0, 4, before))
            for at, part, slot, there in plan:
                place_z = slice(None) if axis == "y" else at
                place_y = at if axis == "y" else slice(None)
                block = partial.at[place_y, high, e, place_z, :, c, :, columns_of(part)]
                into = slots.at[slot, high] if axis == "y" else slots.at[slot, :, high]
                went[e].append(copies.start(block, into, there))
        return went

    def relay(e, axis, whole, slots, low, high):
        after, _, before = around(axis)
        up, down = turned(pos[axis], 1), turned(pos[axis], 3)
        for copy in low:
            copy.wait_recv()
        add(e, axis, up, whole, 0, [slots.at[0]])
        block = region(partial, e, {axis: up}, whole, 0)
        sent = [copies.start(block, slots.at[2], after)]
        for copy in high:
            copy.wait_recv()
        add(e, axis, down, whole, 1, [slots.at[1]])
        block = region(partial, e, {axis: down}, whole, 1)
        return sent + [copies.start(block, slots.at[5], before)]

    def last_sums(e, axis, whole, slots, waits):
        for copy in waits:
            copy.wait_recv()
        for part in range(2):
            add(e, axis, pos[axis], whole, part, [slots.at[2 + part], slots.at[4 + part]])

    first = (first_0, first_1, first_2)
    lax.fori_loop(0, 5, fold, 0)
    lax.fori_loop(0, 4, add_swapped, 0)
    near_half = first_group(0)
    lax.fori_loop(5, 8, fold, 0)
    lax.fori_loop(4, 8, add_swapped, 0)
    own_half = first_group(1)
    lax.fori_loop(0, 5, outer, 0)
    waits = []
    for e in range(EXITS):
        one, two = near_half[e], own_half[e]
        if e == 0:
            low, high, rest = one[:1], one[1:2], one[2:] + two
        else:
            low, high, rest = [one[0], two[0]], [one[1], two[1]], one[2:] + two[2:]
        waits.append(rest + relay(e, ORDER[e][2], ORDER[e][:2], first[e], low, high))
    lax.fori_loop(5, 8, outer, 0)
    for e in range(EXITS):
        last_sums(e, ORDER[e][2], ORDER[e][:2], first[e], waits[e])
    second = (second_0, second_1, second_2)
    began = [first_copies(e, ORDER[e][1], ORDER[e][:1], second[e]) for e in range(EXITS)]
    waits = []
    for e in range(EXITS):
        low, high = began[e][:1], began[e][1:2]
        sent = relay(e, ORDER[e][1], ORDER[e][:1], second[e], low, high)
        waits.append(began[e][2:] + sent)
    for e in range(EXITS):
        last_sums(e, ORDER[e][1], ORDER[e][:1], second[e], waits[e])
    went = []
    for e in range(EXITS):
        axis = ORDER[e][0]
        for k, there in enumerate(around(axis)):
            block = region(partial, e, {axis: turned(pos[axis], k + 1)}, (), None)
            went.append(copies.start(block, third.at[e, k], there))
    inner_sums = []
    for e in range(EXITS):
        total = partial[y, xh, e, z, xl, c].astype(f32)
        for k in range(3):
            went[3 * e + k].wait_recv()
            total = total + third[e, k].astype(f32)
        weighted = gain[e : e + 1, :] * total
        summed[e] = weighted
        inner_sums.append(jnp.sum(weighted * hidden[e].astype(f32), axis=1, keepdims=True))
    inner_slots[s] = by_lane(inner_sums, ROWS)
    to_all(copies, inner_slots, s, section_peers(s, v))
    inner = slots_sum(inner_slots, 8)
    cube = inverse[...] * inverse[...] * inverse[...] * inner / (8 * width)
    for e in range(EXITS):
        scale = column_of(inverse[...], e)
        back = scale * summed[e] - hidden[e].astype(f32) * column_of(cube, e)
        grad_hidden[e] = back.astype(bf16)
    copies.finish()
    for k in range(8):
        exchange(k).wait_send()


def body(exit_hidden, norm_gain, head_weight, teacher):
    width, cols = exit_hidden.shape[2], head_weight.shape[1]
    half = width // 2
    vmem = pl.BlockSpec(memory_space=pltpu.VMEM)
    hbm = pl.BlockSpec(memory_space=pltpu.HBM)
    dma = pltpu.SemaphoreType.DMA
    tile = (4, 2, EXITS, 4, 2, 2, ROWS, width)
    divergence, grad_hidden, grad_head = pl.pallas_call(
        kernel,
        out_shape=(
            jax.ShapeDtypeStruct((EXITS, 128), f32),
            jax.ShapeDtypeStruct(exit_hidden.shape, bf16),
            pltpu.VMEM(head_weight.shape, bf16),
        ),
        in_specs=[hbm] * 4,
        out_specs=(vmem,) * 3,
        scratch_shapes=[
            pltpu.VMEM(exit_hidden.shape, bf16),
            pltpu.VMEM(norm_gain.shape, f32),
            pltpu.VMEM(teacher.shape, f32),
            pltpu.VMEM(tile, bf16),
            pltpu.VMEM(head_weight.shape, bf16),
            pltpu.VMEM((EXITS, 4, 2, 2, ROWS, cols), f32),
            pltpu.VMEM((16, ROWS, cols), f32),
            pltpu.VMEM((EXITS * TOKENS, cols), bf16),
            pltpu.VMEM((ROWS, 128), f32),
            pltpu.VMEM(exit_hidden.shape, f32),
            pltpu.VMEM(tile, bf16),
            pltpu.VMEM((4, 2, EXITS, 4, 2, ROWS, width), bf16),
        ]
        + [
            pltpu.VMEM((6, *(n for _, n in whole_dims(ORDER[e][:whole])), ROWS, half), bf16)
            for whole in (2, 1)
            for e in range(EXITS)
        ]
        + [
            pltpu.VMEM((EXITS, 3, ROWS, width), bf16),
            pltpu.VMEM((8, ROWS, 128), f32),
            pltpu.VMEM((16, 8, TOKENS), f32),
            pltpu.VMEM((8, 8, TOKENS), f32),
            pltpu.VMEM((8, ROWS, 128), f32),
            dma((172,)),
            dma((172,)),
            dma((8,)),
            dma((8,)),
            dma((4,)),
        ],
        compiler_params=pltpu.CompilerParams(
            collective_id=0, has_side_effects=True, vmem_limit_bytes=53 * 2**20
        ),
        name="exits",
    )(exit_hidden, norm_gain, teacher, head_weight)
    return divergence[:, 0], grad_hidden, grad_head


def solution(mesh):
    return jax.shard_map(
        body,
        mesh=mesh,
        in_specs=(
            P(None, "vocab", "section"),
            P(None, "section"),
            P(None, ("section", "vocab")),
            P("vocab", "section"),
        ),
        out_specs=(P(), P(None, "vocab", "section"), P(None, ("section", "vocab"))),
        check_vma=False,
    )
```

```python
import functools

import jax
import jax.numpy as jnp
from jax import lax
from jax.experimental import pallas as pl
from jax.experimental.pallas import tpu as pltpu
from jax.sharding import PartitionSpec as P

MESH = pl.DeviceIdType.MESH
EXITS = 3
ROWS = 16
TOKENS = 256
epsilon = 1e-05
loss_scale = 1024.0
AXES = ("x", "y", "z")
ORDER = (("y", "z", "x"), ("z", "x", "y"), ("x", "y", "z"))
bf16 = jnp.bfloat16
f32 = jnp.float32


def chip(x, y, z, c):
    return (y * 2 + lax.div(x, 2), z * 4 + lax.rem(x, 2) * 2 + c)


def place():
    s, v = lax.axis_index("section"), lax.axis_index("vocab")
    x = lax.rem(s, 2) * 2 + lax.rem(lax.div(v, 2), 2)
    return s, v, dict(x=x, y=lax.div(s, 2), z=lax.div(v, 4)), lax.rem(v, 2)


def turned(k, by):
    return lax.rem(k + by, 4)


class Copies:
    def __init__(self, send_sem, recv_sem):
        self.send_sem, self.recv_sem, self.made, self.left = send_sem, recv_sem, [], 0

    def start(self, src, dst, device):
        n = len(self.made)
        copy = pltpu.make_async_remote_copy(
            src_ref=src,
            dst_ref=dst,
            send_sem=self.send_sem.at[n],
            recv_sem=self.recv_sem.at[n],
            device_id=device,
            device_id_type=MESH,
        )
        copy.start()
        self.made.append(copy)
        return copy

    def finish(self):
        for copy in self.made[self.left :]:
            copy.wait_send()
        self.left = len(self.made)


def neighbour(pos, c, axis, by):
    there = dict(pos)
    there[axis] = turned(pos[axis], by)
    return chip(**there, c=c)


def greet(devices):
    barrier = pltpu.get_barrier_semaphore()
    for device in devices:
        pl.semaphore_signal(barrier, inc=1, device_id=device, device_id_type=MESH)
    return lambda: pl.semaphore_wait(barrier, len(devices))


def section_peers(s, v):
    return [(lax.rem(s + k, 8), v) for k in range(1, 8)]


def vocab_peers(s, v):
    return [(s, lax.rem(v + k, 16)) for k in range(1, 16)]


DIMS = (("y", 4), ("xh", 2), ("z", 4), ("xl", 2))


def split_x(pos):
    return {
        "y": pos["y"],
        "xh": lax.div(pos["x"], 2),
        "z": pos["z"],
        "xl": lax.rem(pos["x"], 2),
    }


def whole_dims(whole):
    return [(d, n) for d, n in DIMS if d[0] in whole]


def begin(copies, slots, me, peers):
    return [copies.start(slots.at[me], slots.at[me], peer) for peer in peers]


def wait_for(sent):
    for copy in sent:
        copy.wait_recv()


def to_all(copies, slots, me, peers):
    wait_for(begin(copies, slots, me, peers))


def by_lane(columns, rows):
    lane = lax.broadcasted_iota(jnp.int32, (rows, 128), 1)
    tile = jnp.zeros((rows, 128), f32)
    for k, column in enumerate(columns):
        tile = jnp.where(lane == k, column, tile)
    return tile


def column_of(tile, k):
    lane = lax.broadcasted_iota(jnp.int32, tile.shape, 1)
    return jnp.sum(jnp.where(lane == k, tile, 0.0), axis=1, keepdims=True)


def slots_sum(slots, count):
    total = slots[0]
    for k in range(1, count):
        total = total + slots[k]
    return total


def merged(slots, count):
    top = slots[0]
    for k in range(1, count):
        top = jnp.maximum(top, slots[k])
    exps = jnp.zeros(top.shape, f32)
    sums = jnp.zeros(top.shape, f32)
    for k in range(count):
        part = slots[k]
        exps = exps + jnp.exp(part - top)
        sums = sums + part
    row = lax.broadcasted_iota(jnp.int32, top.shape, 0)
    return jnp.where(row < EXITS, top + jnp.log(exps), sums)


def kernel(
    hidden_hbm, gain_hbm, teacher_hbm, head_hbm, divergence, grad_hidden, grad_head,
    hidden, gain, teacher, full, head, logits, target, dlogit, inverse, partial, swapped,
    first_0, first_1, first_2, second_0, second_1, second_2, third,
    square_slots, vocab_slots, section_slots, gain_slots, inverse_slots, inner_vocab, inner_section,
    inner_rows,
    send_sem, recv_sem, swap_send, swap_recv, local_sem,
):
    width, cols = hidden.shape[2], head.shape[1]
    half = width // 2
    s, v, pos, c = place()
    x, y, z = pos["x"], pos["y"], pos["z"]
    xh, xl = lax.div(x, 2), lax.rem(x, 2)
    partner = chip(**pos, c=1 - c)
    copies = Copies(send_sem, recv_sem)
    same_core = [(s, lax.rem(v + k, 16)) for k in range(2, 16, 2)]
    beyond = neighbour(pos, c, "x", 3 + 2 * xl)
    ready = greet([partner, beyond] + section_peers(s, v) + same_core)
    loads = [
        pltpu.make_async_copy(src, dst, local_sem.at[k])
        for k, (src, dst) in enumerate(
            ((hidden_hbm, hidden), (gain_hbm, gain), (head_hbm, head), (teacher_hbm, teacher))
        )
    ]
    for load in loads:
        load.start()
    loads[0].wait()
    squares = [
        jnp.sum(jnp.square(hidden[e].astype(f32)), axis=1, keepdims=True) for e in range(EXITS)
    ]
    square_slots[s] = by_lane(squares, ROWS)
    for e in range(EXITS):
        full[y, xh, e, z, xl, c] = hidden[e]
    loads[1].wait()
    gain_slots[s] = gain[...]
    ready()
    square_copies = begin(copies, square_slots, s, section_peers(s, v))

    def columns_of(part):
        return slice(None) if part is None else slice(part * half, (part + 1) * half)

    def region(ref, e, over, whole, part):
        at = split_x({**pos, **over})
        for d, _ in whole_dims(whole):
            at[d] = slice(None)
        return ref.at[at["y"], at["xh"], e, at["z"], at["xl"], c, :, columns_of(part)]

    def around(axis):
        return [neighbour(pos, c, axis, by) for by in (1, 2, 3)]

    def swap(ref):
        return copies.start(ref, ref, partner)

    def rows_of(k):
        return full[lax.div(k, 2), lax.rem(k, 2)].reshape(EXITS * TOKENS, width)

    def head_rows(k):
        return pl.ds(pl.multiple_of(k * width, 128), width)

    def across_x(by):
        there = turned(x, by)
        high, low = lax.div(there, 2), lax.rem(there, 2)

        def step(k, _):
            tokens = full[k, high, 0, :, low].reshape(TOKENS // 2, width)
            part = jnp.dot(tokens, head[head_rows(2 * k + high), :], preferred_element_type=f32)
            logits[0, :, low] += part.reshape(4, 2, ROWS, cols)
            return 0

        lax.fori_loop(0, 4, step, 0)

    def across_y(by):
        there = turned(y, by)

        def step(k, _):
            tokens = full[there, k, 1].reshape(TOKENS, width)
            part = jnp.dot(tokens, head[head_rows(2 * there + k), :], preferred_element_type=f32)
            logits[1] += part.reshape(4, 2, 2, ROWS, cols)
            return 0

        lax.fori_loop(0, 2, step, 0)

    def last_exit(k, _):
        tokens = full[lax.div(k, 2), lax.rem(k, 2), 2].reshape(TOKENS, width)
        part = jnp.dot(tokens, head[head_rows(k), :], preferred_element_type=f32)
        logits[2] += part.reshape(4, 2, 2, ROWS, cols)
        return 0

    logits[...] = jnp.zeros(logits.shape, f32)

    sent = []
    for e in range(EXITS):
        mine = region(full, e, {}, (), None)
        sent += [copies.start(mine, mine, there) for there in around(ORDER[e][0])]
    gain_copies = [copies.start(gain, gain_slots.at[s], peer) for peer in section_peers(s, v)]
    wait_for(sent)

    def normalise(block, scale, gains):
        block[...] = (block[...].astype(f32) * scale * gains).astype(bf16)

    def normalise_step(k, _):
        for n in range(4):
            high, low = divmod(n, 2)
            normalise(
                full.at[k, xh, 0, n, xl, c],
                inverse_slots[2 * n + xl][:, 0:1],
                gain_slots[2 * k + xh][0:1, :],
            )
            normalise(
                full.at[y, high, 1, k, low, c],
                inverse_slots[2 * k + low][:, 1:2],
                gain_slots[2 * y + high][1:2, :],
            )
            normalise(
                full.at[k, high, 2, z, low, c],
                inverse_slots[2 * z + low][:, 2:3],
                gain_slots[2 * k + high][2:3, :],
            )
        return 0

    for turn in (1, 2):
        last = turn == 2
        pieces = []
        if last:
            wait_for(gain_copies + inverse_copies)
            copies.finish()
            lax.fori_loop(0, 4, normalise_step, 0)
        for e in range(EXITS):
            axis, whole = ORDER[e][turn], ORDER[e][:turn]
            after, _, before = around(axis)
            low, high = region(full, e, {}, whole, 0), region(full, e, {}, whole, 1)
            up_low = copies.start(low, low, after)
            down_high = copies.start(high, high, before)
            up_high = copies.start(high, high, after)
            down_low = copies.start(low, low, before)
            pieces.append((up_low, down_high, up_high, down_low))
        if last:
            own_swaps = [swap(region(full, e, {}, ORDER[e][:2], None)) for e in range(EXITS)]
            near_swaps = [[], [], []]
            far_swaps = [[], [], [own_swaps[2]]]
            loads[2].wait()
            for e in range(2):
                own_swaps[e].wait_recv()
                (across_x, across_y)[e](0)
        else:
            wait_for(square_copies)
            inverse[...] = lax.rsqrt(slots_sum(square_slots, 8) / (8 * width) + epsilon)
            inverse_slots[lax.div(v, 2)] = inverse[...]
            inverse_copies = begin(copies, inverse_slots, lax.div(v, 2), same_core)
        relays = []
        for e in range(EXITS):
            axis, whole = ORDER[e][turn], ORDER[e][:turn]
            after, _, before = around(axis)
            up_low, down_high, _, _ = pieces[e]
            up_low.wait_recv()
            block = region(full, e, {axis: turned(pos[axis], 3)}, whole, 0)
            up = copies.start(block, block, after)
            if last:
                near_swaps[e].append(swap(block))
            down_high.wait_recv()
            block = region(full, e, {axis: turned(pos[axis], 1)}, whole, 1)
            down = copies.start(block, block, before)
            if last:
                near_swaps[e].append(swap(block))
            relays.append((up, down))
        for e in range(EXITS):
            axis, whole = ORDER[e][turn], ORDER[e][:turn]
            pieces[e][2].wait_recv()
            if last:
                near_swaps[e].append(swap(region(full, e, {axis: turned(pos[axis], 3)}, whole, 1)))
            pieces[e][3].wait_recv()
            if last:
                near_swaps[e].append(swap(region(full, e, {axis: turned(pos[axis], 1)}, whole, 0)))
        if last:
            loads[3].wait()
            lent = [
                copies.start(
                    teacher.at[:, pl.ds(pl.multiple_of(peer[1] * cols, 128), cols)],
                    target.at[v],
                    peer,
                )
                for peer in vocab_peers(s, v)
            ]
            target[v] = teacher[:, pl.ds(pl.multiple_of(v * cols, 128), cols)]
            for e in range(2):
                for copy in near_swaps[e]:
                    copy.wait_recv()
                (across_x, across_y)[e](1)
                (across_x, across_y)[e](3)
            far_swaps[2] += near_swaps[2]
        for e in range(EXITS):
            axis, whole = ORDER[e][turn], ORDER[e][:turn]
            for k in range(2):
                relays[e][k].wait_recv()
                if last:
                    block = region(full, e, {axis: turned(pos[axis], 2)}, whole, k)
                    far_swaps[e].append(swap(block))
    for e in range(EXITS):
        axis, whole = ORDER[e][2], ORDER[e][:2]
        for copy in far_swaps[e]:
            copy.wait_recv()
        if e < 2:
            (across_x, across_y)[e](2)
    lax.fori_loop(0, 8, last_exit, 0)
    for copy in lent:
        copy.wait_recv()

    columns = []
    for e in range(EXITS):
        block = logits[e].reshape(TOKENS, cols)
        top = jnp.max(block, axis=1, keepdims=True)
        columns.append(top + jnp.log(jnp.sum(jnp.exp(block - top), axis=1, keepdims=True)))
    stored = target[...].reshape(TOKENS, cols)
    weight = jnp.exp(stored)
    for e in range(EXITS):
        block = logits[e].reshape(TOKENS, cols)
        columns.append(jnp.sum(weight * (stored - block), axis=1, keepdims=True))
    columns.append(jnp.sum(weight, axis=1, keepdims=True))
    vocab_slots[v] = jnp.transpose(by_lane(columns, TOKENS))[:8]
    to_all(copies, vocab_slots, v, vocab_peers(s, v))
    section_slots[s] = merged(vocab_slots, 16)
    to_all(copies, section_slots, s, section_peers(s, v))
    rows = merged(section_slots, 8)
    turned_rows = jnp.transpose(jnp.concatenate([rows, jnp.zeros((120, TOKENS), f32)], axis=0))
    for e in range(EXITS):
        block = logits[e].reshape(TOKENS, cols)
        log_total = turned_rows[:, e : e + 1]
        grad = (jnp.exp(block - log_total) - weight) * (loss_scale / TOKENS)
        dlogit[e * TOKENS : (e + 1) * TOKENS, :] = grad.astype(bf16)

    def fold_place(k):
        return lax.rem(y + lax.rem(k, 4), 4), lax.rem(xh + 1 - lax.div(k, 4), 2)

    def exchange(k):
        yk, xk = fold_place(k)
        return pltpu.make_async_remote_copy(
            src_ref=partial.at[yk, xk, :, :, :, 1 - c],
            dst_ref=swapped.at[yk, xk],
            send_sem=swap_send.at[k],
            recv_sem=swap_recv.at[k],
            device_id=partner,
            device_id_type=MESH,
        )

    def fold(k, _):
        yk, xk = fold_place(k)
        rows = head[head_rows(2 * yk + xk), :]
        part = lax.dot_general(
            dlogit[...], rows, (((1,), (1,)), ((), ())), preferred_element_type=f32
        )
        shape = (EXITS, 4, 2, 2, ROWS, width)
        partial[yk, xk] = part.astype(bf16).reshape(shape)
        exchange(k).start()
        return 0

    def add_swapped(k, _):
        yk, xk = fold_place(k)
        exchange(k).wait_recv()
        for e in range(EXITS):
            for low in range(2):
                mine = partial[yk, xk, e, :, low, c].astype(f32)
                theirs = swapped[yk, xk, e, :, low].astype(f32)
                partial[yk, xk, e, :, low, c] = (mine + theirs).astype(bf16)
        return 0

    def outer(k, _):
        part = lax.dot_general(
            rows_of(k), dlogit[...], (((0,), (0,)), ((), ())), preferred_element_type=f32
        )
        grad_head[head_rows(k), :] = part.astype(bf16)
        return 0

    terms = rows[EXITS : 2 * EXITS] + rows[:EXITS] * rows[2 * EXITS : 2 * EXITS + 1]
    mean = jnp.sum(terms, axis=1, keepdims=True) / TOKENS
    divergence[...] = jnp.broadcast_to(mean, (EXITS, 128))

    def add(e, axis, at, whole, part, arrived):
        dims = whole_dims(whole)

        def step(n, _):
            index = split_x({**pos, axis: at})
            found = []
            for d, size in reversed(dims):
                index[d] = lax.rem(n, size)
                found.insert(0, index[d])
                n = lax.div(n, size)
            ref = partial.at[
                index["y"], index["xh"], e, index["z"], index["xl"], c, :, columns_of(part)
            ]
            total = ref[...].astype(f32)
            for slot in arrived:
                total = total + slot[tuple(found)].astype(f32)
            ref[...] = total.astype(bf16)
            return 0

        lax.fori_loop(0, 4 ** len(whole), step, 0)

    def first_copies(e, axis, whole, slots):
        after, _, before = around(axis)
        up, far, down = (turned(pos[axis], k) for k in (1, 2, 3))
        return [
            copies.start(region(partial, e, {axis: far}, whole, 0), slots.at[0], after),
            copies.start(region(partial, e, {axis: far}, whole, 1), slots.at[1], before),
            copies.start(region(partial, e, {axis: up}, whole, 1), slots.at[3], after),
            copies.start(region(partial, e, {axis: down}, whole, 0), slots.at[4], before),
        ]

    def first_group(group):
        high = lax.rem(xh + 1 - group, 2)
        went = [[], [], []]
        if group == 0:
            after, _, before = around("x")
            for part, there in ((0, after), (1, before)):
                block = region(partial, 0, {"x": turned(x, 2)}, ("y", "z"), part)
                went[0].append(copies.start(block, first_0.at[part], there))
        side = xl if group == 0 else 1 - xl
        by = 3 + 2 * side
        block = partial.at[
            :, high, 0, :, 1 - xl, c, :, pl.ds(pl.multiple_of(side * half, 128), half)
        ]
        went[0].append(copies.start(block, first_0.at[4 - side], neighbour(pos, c, "x", by)))
        for e, axis, slots in ((1, "y", first_1), (2, "z", first_2)):
            after, _, before = around(axis)
            up, far, down = (turned(pos[axis], k) for k in (1, 2, 3))
            plan = ((far, 0, 0, after), (far, 1, 1, before), (up, 1, 3, after), (down, 0, 4, before))
            for at, part, slot, there in plan:
                place_z = slice(None) if axis == "y" else at
                place_y = at if axis == "y" else slice(None)
                block = partial.at[place_y, high, e, place_z, :, c, :, columns_of(part)]
                into = slots.at[slot, high] if axis == "y" else slots.at[slot, :, high]
                went[e].append(copies.start(block, into, there))
        return went

    def relay(e, axis, whole, slots, low, high):
        after, _, before = around(axis)
        up, down = turned(pos[axis], 1), turned(pos[axis], 3)
        for copy in low:
            copy.wait_recv()
        add(e, axis, up, whole, 0, [slots.at[0]])
        block = region(partial, e, {axis: up}, whole, 0)
        sent = [copies.start(block, slots.at[2], after)]
        for copy in high:
            copy.wait_recv()
        add(e, axis, down, whole, 1, [slots.at[1]])
        block = region(partial, e, {axis: down}, whole, 1)
        return sent + [copies.start(block, slots.at[5], before)]

    def last_sums(e, axis, whole, slots, waits):
        for copy in waits:
            copy.wait_recv()
        for part in range(2):
            add(e, axis, pos[axis], whole, part, [slots.at[2 + part], slots.at[4 + part]])

    first = (first_0, first_1, first_2)
    lax.fori_loop(0, 5, fold, 0)
    lax.fori_loop(0, 4, add_swapped, 0)
    near_half = first_group(0)
    lax.fori_loop(5, 8, fold, 0)
    lax.fori_loop(4, 8, add_swapped, 0)
    own_half = first_group(1)
    columns = []
    for e in range(EXITS):
        grad = dlogit[e * TOKENS : (e + 1) * TOKENS, :].astype(f32)
        columns.append(jnp.sum(grad * logits[e].reshape(TOKENS, cols), axis=1, keepdims=True))
    inner_vocab[v] = jnp.transpose(by_lane(columns, TOKENS))[:8]
    inner_copies = begin(copies, inner_vocab, v, vocab_peers(s, v))
    lax.fori_loop(0, 5, outer, 0)
    wait_for(inner_copies)
    inner_section[s] = slots_sum(inner_vocab, 16)
    inner_copies = begin(copies, inner_section, s, section_peers(s, v))
    waits = []
    for e in range(EXITS):
        one, two = near_half[e], own_half[e]
        if e == 0:
            low, high, rest = one[:1], one[1:2], one[2:] + two
        else:
            low, high, rest = [one[0], two[0]], [one[1], two[1]], one[2:] + two[2:]
        waits.append(rest + relay(e, ORDER[e][2], ORDER[e][:2], first[e], low, high))
    lax.fori_loop(5, 8, outer, 0)
    for e in range(EXITS):
        last_sums(e, ORDER[e][2], ORDER[e][:2], first[e], waits[e])
    wait_for(inner_copies)
    inner = slots_sum(inner_section, 8)
    inner_rows[...] = jnp.transpose(jnp.concatenate([inner, jnp.zeros((120, TOKENS), f32)], axis=0))
    second = (second_0, second_1, second_2)
    began = [first_copies(e, ORDER[e][1], ORDER[e][:1], second[e]) for e in range(EXITS)]
    waits = []
    for e in range(EXITS):
        low, high = began[e][:1], began[e][1:2]
        sent = relay(e, ORDER[e][1], ORDER[e][:1], second[e], low, high)
        waits.append(began[e][2:] + sent)
    for e in range(EXITS):
        last_sums(e, ORDER[e][1], ORDER[e][:1], second[e], waits[e])
    own_inner = inner_rows[pl.ds(pl.multiple_of(v * ROWS, ROWS), ROWS), :]
    removed = inverse[...] * inverse[...] * own_inner / (8 * width)
    went = []
    for e in range(EXITS):
        axis = ORDER[e][0]
        for k, there in enumerate(around(axis)):
            block = region(partial, e, {axis: turned(pos[axis], k + 1)}, (), None)
            went.append(copies.start(block, third.at[e, k], there))
    for e in range(EXITS):
        total = partial[y, xh, e, z, xl, c].astype(f32)
        for k in range(3):
            went[3 * e + k].wait_recv()
            total = total + third[e, k].astype(f32)
        scale = column_of(inverse[...], e)
        back = scale * (gain[e : e + 1, :] * total) - hidden[e].astype(f32) * column_of(removed, e)
        grad_hidden[e] = back.astype(bf16)
    copies.finish()
    for k in range(8):
        exchange(k).wait_send()


def body(exit_hidden, norm_gain, head_weight, teacher):
    width, cols = exit_hidden.shape[2], head_weight.shape[1]
    half = width // 2
    vmem = pl.BlockSpec(memory_space=pltpu.VMEM)
    hbm = pl.BlockSpec(memory_space=pltpu.HBM)
    dma = pltpu.SemaphoreType.DMA
    tile = (4, 2, EXITS, 4, 2, 2, ROWS, width)
    divergence, grad_hidden, grad_head = pl.pallas_call(
        kernel,
        out_shape=(
            jax.ShapeDtypeStruct((EXITS, 128), f32),
            jax.ShapeDtypeStruct(exit_hidden.shape, bf16),
            pltpu.VMEM(head_weight.shape, bf16),
        ),
        in_specs=[hbm] * 4,
        out_specs=(vmem,) * 3,
        scratch_shapes=[
            pltpu.VMEM(exit_hidden.shape, bf16),
            pltpu.VMEM(norm_gain.shape, f32),
            pltpu.VMEM(teacher.shape, f32),
            pltpu.VMEM(tile, bf16),
            pltpu.VMEM(head_weight.shape, bf16),
            pltpu.VMEM((EXITS, 4, 2, 2, ROWS, cols), f32),
            pltpu.VMEM((16, ROWS, cols), f32),
            pltpu.VMEM((EXITS * TOKENS, cols), bf16),
            pltpu.VMEM((ROWS, 128), f32),
            pltpu.VMEM(tile, bf16),
            pltpu.VMEM((4, 2, EXITS, 4, 2, ROWS, width), bf16),
        ]
        + [
            pltpu.VMEM((6, *(n for _, n in whole_dims(ORDER[e][:whole])), ROWS, half), bf16)
            for whole in (2, 1)
            for e in range(EXITS)
        ]
        + [
            pltpu.VMEM((EXITS, 3, ROWS, width), bf16),
            pltpu.VMEM((8, ROWS, 128), f32),
            pltpu.VMEM((16, 8, TOKENS), f32),
            pltpu.VMEM((8, 8, TOKENS), f32),
            pltpu.VMEM((8, *norm_gain.shape), f32),
            pltpu.VMEM((8, ROWS, 128), f32),
            pltpu.VMEM((16, 8, TOKENS), f32),
            pltpu.VMEM((8, 8, TOKENS), f32),
            pltpu.VMEM((TOKENS, 128), f32),
            dma((199,)),
            dma((199,)),
            dma((8,)),
            dma((8,)),
            dma((4,)),
        ],
        compiler_params=pltpu.CompilerParams(
            collective_id=0, has_side_effects=True, vmem_limit_bytes=53 * 2**20
        ),
        name="exits",
    )(exit_hidden, norm_gain, teacher, head_weight)
    return divergence[:, 0], grad_hidden, grad_head


def solution(mesh):
    return jax.shard_map(
        body,
        mesh=mesh,
        in_specs=(
            P(None, "vocab", "section"),
            P(None, "section"),
            P(None, ("section", "vocab")),
            P("vocab", "section"),
        ),
        out_specs=(P(), P(None, "vocab", "section"), P(None, ("section", "vocab"))),
        check_vma=False,
    )
```

```python
import functools

import jax
import jax.numpy as jnp
from jax import lax
from jax.experimental import pallas as pl
from jax.experimental.pallas import tpu as pltpu
from jax.sharding import PartitionSpec as P

MESH = pl.DeviceIdType.MESH
EXITS = 3
ROWS = 16
TOKENS = 256
epsilon = 1e-05
loss_scale = 1024.0
AXES = ("x", "y", "z")
ORDER = (("y", "z", "x"), ("z", "x", "y"), ("x", "y", "z"))
bf16 = jnp.bfloat16
f32 = jnp.float32


def chip(x, y, z, c):
    return (y * 2 + lax.div(x, 2), z * 4 + lax.rem(x, 2) * 2 + c)


def place():
    s, v = lax.axis_index("section"), lax.axis_index("vocab")
    x = lax.rem(s, 2) * 2 + lax.rem(lax.div(v, 2), 2)
    return s, v, dict(x=x, y=lax.div(s, 2), z=lax.div(v, 4)), lax.rem(v, 2)


def turned(k, by):
    return lax.rem(k + by, 4)


class Copies:
    def __init__(self, send_sem, recv_sem):
        self.send_sem, self.recv_sem, self.made, self.left = send_sem, recv_sem, [], 0

    def start(self, src, dst, device):
        n = len(self.made)
        copy = pltpu.make_async_remote_copy(
            src_ref=src,
            dst_ref=dst,
            send_sem=self.send_sem.at[n],
            recv_sem=self.recv_sem.at[n],
            device_id=device,
            device_id_type=MESH,
        )
        copy.start()
        self.made.append(copy)
        return copy

    def finish(self):
        for copy in self.made[self.left :]:
            copy.wait_send()
        self.left = len(self.made)


def neighbour(pos, c, axis, by):
    there = dict(pos)
    there[axis] = turned(pos[axis], by)
    return chip(**there, c=c)


def greet(devices):
    barrier = pltpu.get_barrier_semaphore()
    for device in devices:
        pl.semaphore_signal(barrier, inc=1, device_id=device, device_id_type=MESH)
    return lambda: pl.semaphore_wait(barrier, len(devices))


def section_peers(s, v):
    return [(lax.rem(s + k, 8), v) for k in range(1, 8)]


def vocab_peers(s, v):
    return [(s, lax.rem(v + k, 16)) for k in range(1, 16)]


DIMS = (("y", 4), ("xh", 2), ("z", 4), ("xl", 2))


def split_x(pos):
    return {
        "y": pos["y"],
        "xh": lax.div(pos["x"], 2),
        "z": pos["z"],
        "xl": lax.rem(pos["x"], 2),
    }


def whole_dims(whole):
    return [(d, n) for d, n in DIMS if d[0] in whole]


def begin(copies, slots, me, peers):
    return [copies.start(slots.at[me], slots.at[me], peer) for peer in peers]


def wait_for(sent):
    for copy in sent:
        copy.wait_recv()


def to_all(copies, slots, me, peers):
    wait_for(begin(copies, slots, me, peers))


def by_lane(columns, rows):
    lane = lax.broadcasted_iota(jnp.int32, (rows, 128), 1)
    tile = jnp.zeros((rows, 128), f32)
    for k, column in enumerate(columns):
        tile = jnp.where(lane == k, column, tile)
    return tile


def column_of(tile, k):
    lane = lax.broadcasted_iota(jnp.int32, tile.shape, 1)
    return jnp.sum(jnp.where(lane == k, tile, 0.0), axis=1, keepdims=True)


def slots_sum(slots, count):
    total = slots[0]
    for k in range(1, count):
        total = total + slots[k]
    return total


def merged(slots, count):
    top = slots[0]
    for k in range(1, count):
        top = jnp.maximum(top, slots[k])
    exps = jnp.zeros(top.shape, f32)
    sums = jnp.zeros(top.shape, f32)
    for k in range(count):
        part = slots[k]
        exps = exps + jnp.exp(part - top)
        sums = sums + part
    row = lax.broadcasted_iota(jnp.int32, top.shape, 0)
    return jnp.where(row < EXITS, top + jnp.log(exps), sums)


def kernel(
    hidden_hbm, gain_hbm, teacher_hbm, head_hbm, divergence, grad_hidden, grad_head,
    hidden, gain, teacher, full, head, logits, target, dlogit, inverse, partial, swapped,
    first_0, first_1, first_2, second_0, second_1, second_2, third,
    square_slots, vocab_slots, section_slots, gain_slots, inverse_slots, inner_vocab, inner_section,
    inner_rows,
    send_sem, recv_sem, swap_send, swap_recv, local_sem,
):
    width, cols = hidden.shape[2], head.shape[1]
    half = width // 2
    s, v, pos, c = place()
    x, y, z = pos["x"], pos["y"], pos["z"]
    xh, xl = lax.div(x, 2), lax.rem(x, 2)
    partner = chip(**pos, c=1 - c)
    copies = Copies(send_sem, recv_sem)
    same_core = [(s, lax.rem(v + k, 16)) for k in range(2, 16, 2)]
    beyond = neighbour(pos, c, "x", 3 + 2 * xl)
    ready = greet([partner, beyond] + section_peers(s, v) + same_core)
    loads = [
        pltpu.make_async_copy(src, dst, local_sem.at[k])
        for k, (src, dst) in enumerate(
            ((hidden_hbm, hidden), (gain_hbm, gain), (head_hbm, head), (teacher_hbm, teacher))
        )
    ]
    for load in loads:
        load.start()
    loads[0].wait()
    squares = [
        jnp.sum(jnp.square(hidden[e].astype(f32)), axis=1, keepdims=True) for e in range(EXITS)
    ]
    square_slots[s] = by_lane(squares, ROWS)
    for e in range(EXITS):
        full[y, xh, e, z, xl, c] = hidden[e]
    loads[1].wait()
    gain_slots[s] = gain[...]
    ready()
    square_copies = begin(copies, square_slots, s, section_peers(s, v))

    def columns_of(part):
        return slice(None) if part is None else slice(part * half, (part + 1) * half)

    def region(ref, e, over, whole, part):
        at = split_x({**pos, **over})
        for d, _ in whole_dims(whole):
            at[d] = slice(None)
        return ref.at[at["y"], at["xh"], e, at["z"], at["xl"], c, :, columns_of(part)]

    def around(axis):
        return [neighbour(pos, c, axis, by) for by in (1, 2, 3)]

    def swap(ref):
        return copies.start(ref, ref, partner)

    def rows_of(k):
        return full[lax.div(k, 2), lax.rem(k, 2)].reshape(EXITS * TOKENS, width)

    def head_rows(k):
        return pl.ds(pl.multiple_of(k * width, 128), width)

    def across_x(by):
        there = turned(x, by)
        high, low = lax.div(there, 2), lax.rem(there, 2)

        def step(k, _):
            tokens = full[k, high, 0, :, low].reshape(TOKENS // 2, width)
            part = jnp.dot(tokens, head[head_rows(2 * k + high), :], preferred_element_type=f32)
            logits[0, :, low] += part.reshape(4, 2, ROWS, cols)
            return 0

        lax.fori_loop(0, 4, step, 0)

    def across_y(by):
        there = turned(y, by)

        def step(k, _):
            tokens = full[there, k, 1].reshape(TOKENS, width)
            part = jnp.dot(tokens, head[head_rows(2 * there + k), :], preferred_element_type=f32)
            logits[1] += part.reshape(4, 2, 2, ROWS, cols)
            return 0

        lax.fori_loop(0, 2, step, 0)

    def last_exit(k, _):
        yk, xk = lax.div(k, 2), lax.rem(k, 2)
        places = [z, turned(z, 1), turned(z, 3)]
        tokens = [full[yk, xk, 2, at].reshape(TOKENS // 4, width) for at in places]
        rows = head[head_rows(k), :]
        part = jnp.dot(jnp.concatenate(tokens, axis=0), rows, preferred_element_type=f32)
        part = part.reshape(3, 2, 2, ROWS, cols)
        for n, at in enumerate(places):
            logits[2, at] += part[n]
        return 0

    def far_blocks(yk, xk, with_y, with_x):
        far_x, far_z = turned(x, 2), turned(z, 2)
        low = lax.rem(far_x, 2)
        tokens = [full[yk, xk, 2, far_z].reshape(TOKENS // 4, width)]
        if with_x:
            tokens.append(full[yk, xk, 0, :, low].reshape(TOKENS // 2, width))
        if with_y:
            tokens.append(full[yk, xk, 1].reshape(TOKENS, width))
        tokens = jnp.concatenate(tokens, axis=0) if len(tokens) > 1 else tokens[0]
        part = jnp.dot(tokens, head[head_rows(2 * yk + xk), :], preferred_element_type=f32)
        at = TOKENS // 4
        logits[2, far_z] += part[:at].reshape(2, 2, ROWS, cols)
        if with_x:
            logits[0, :, low] += part[at : at + TOKENS // 2].reshape(4, 2, ROWS, cols)
            at += TOKENS // 2
        if with_y:
            logits[1] += part[at:].reshape(4, 2, 2, ROWS, cols)

    def far_step(k, _):
        yk = turned(y, 3 + k)
        far_blocks(yk, 1 - xh, False, True)
        far_blocks(yk, xh, False, False)
        return 0

    logits[...] = jnp.zeros(logits.shape, f32)

    sent = []
    for e in range(EXITS):
        mine = region(full, e, {}, (), None)
        sent += [copies.start(mine, mine, there) for there in around(ORDER[e][0])]
    gain_copies = [copies.start(gain, gain_slots.at[s], peer) for peer in section_peers(s, v)]
    wait_for(sent)

    def normalise(block, scale, gains):
        block[...] = (block[...].astype(f32) * scale * gains).astype(bf16)

    def normalise_step(k, _):
        for n in range(4):
            high, low = divmod(n, 2)
            normalise(
                full.at[k, xh, 0, n, xl, c],
                inverse_slots[2 * n + xl][:, 0:1],
                gain_slots[2 * k + xh][0:1, :],
            )
            normalise(
                full.at[y, high, 1, k, low, c],
                inverse_slots[2 * k + low][:, 1:2],
                gain_slots[2 * y + high][1:2, :],
            )
            normalise(
                full.at[k, high, 2, z, low, c],
                inverse_slots[2 * z + low][:, 2:3],
                gain_slots[2 * k + high][2:3, :],
            )
        return 0

    for turn in (1, 2):
        last = turn == 2
        pieces = []
        if last:
            wait_for(gain_copies + inverse_copies)
            copies.finish()
            lax.fori_loop(0, 4, normalise_step, 0)
        for e in range(EXITS):
            axis, whole = ORDER[e][turn], ORDER[e][:turn]
            after, _, before = around(axis)
            low, high = region(full, e, {}, whole, 0), region(full, e, {}, whole, 1)
            up_low = copies.start(low, low, after)
            down_high = copies.start(high, high, before)
            up_high = copies.start(high, high, after)
            down_low = copies.start(low, low, before)
            pieces.append((up_low, down_high, up_high, down_low))
        if last:
            own_swaps = [swap(region(full, e, {}, ORDER[e][:2], None)) for e in range(EXITS)]
            near_swaps = [[], [], []]
            far_swaps = []
            loads[2].wait()
            for e in range(2):
                own_swaps[e].wait_recv()
                (across_x, across_y)[e](0)
        else:
            wait_for(square_copies)
            inverse[...] = lax.rsqrt(slots_sum(square_slots, 8) / (8 * width) + epsilon)
            inverse_slots[lax.div(v, 2)] = inverse[...]
            inverse_copies = begin(copies, inverse_slots, lax.div(v, 2), same_core)
        relays = []
        for e in range(EXITS):
            axis, whole = ORDER[e][turn], ORDER[e][:turn]
            after, _, before = around(axis)
            up_low, down_high, _, _ = pieces[e]
            up_low.wait_recv()
            block = region(full, e, {axis: turned(pos[axis], 3)}, whole, 0)
            up = copies.start(block, block, after)
            if last:
                near_swaps[e].append(swap(block))
            down_high.wait_recv()
            block = region(full, e, {axis: turned(pos[axis], 1)}, whole, 1)
            down = copies.start(block, block, before)
            if last:
                near_swaps[e].append(swap(block))
            relays.append((up, down))
        for e in range(EXITS):
            axis, whole = ORDER[e][turn], ORDER[e][:turn]
            pieces[e][2].wait_recv()
            if last:
                near_swaps[e].append(swap(region(full, e, {axis: turned(pos[axis], 3)}, whole, 1)))
            pieces[e][3].wait_recv()
            if last:
                near_swaps[e].append(swap(region(full, e, {axis: turned(pos[axis], 1)}, whole, 0)))
        if last:
            loads[3].wait()
            lent = [
                copies.start(
                    teacher.at[:, pl.ds(pl.multiple_of(peer[1] * cols, 128), cols)],
                    target.at[v],
                    peer,
                )
                for peer in vocab_peers(s, v)
            ]
            target[v] = teacher[:, pl.ds(pl.multiple_of(v * cols, 128), cols)]
            for e in range(2):
                for copy in near_swaps[e]:
                    copy.wait_recv()
                (across_x, across_y)[e](1)
                (across_x, across_y)[e](3)
            wait_for([own_swaps[2]] + near_swaps[2])
            lax.fori_loop(0, 4, last_exit, 0)
        for e in range(EXITS):
            axis, whole = ORDER[e][turn], ORDER[e][:turn]
            for k in range(2):
                relays[e][k].wait_recv()
                if last:
                    block = region(full, e, {axis: turned(pos[axis], 2)}, whole, k)
                    far_swaps.append(swap(block))
    lax.fori_loop(4, 8, last_exit, 0)
    wait_for(far_swaps)
    far_blocks(turned(y, 2), 1 - xh, True, True)
    far_blocks(turned(y, 2), xh, True, False)
    lax.fori_loop(0, 3, far_step, 0)
    for copy in lent:
        copy.wait_recv()

    columns = []
    for e in range(EXITS):
        block = logits[e].reshape(TOKENS, cols)
        top = jnp.max(block, axis=1, keepdims=True)
        columns.append(top + jnp.log(jnp.sum(jnp.exp(block - top), axis=1, keepdims=True)))
    stored = target[...].reshape(TOKENS, cols)
    weight = jnp.exp(stored)
    for e in range(EXITS):
        block = logits[e].reshape(TOKENS, cols)
        columns.append(jnp.sum(weight * (stored - block), axis=1, keepdims=True))
    columns.append(jnp.sum(weight, axis=1, keepdims=True))
    vocab_slots[v] = jnp.transpose(by_lane(columns, TOKENS))[:8]
    to_all(copies, vocab_slots, v, vocab_peers(s, v))
    section_slots[s] = merged(vocab_slots, 16)
    to_all(copies, section_slots, s, section_peers(s, v))
    rows = merged(section_slots, 8)
    turned_rows = jnp.transpose(jnp.concatenate([rows, jnp.zeros((120, TOKENS), f32)], axis=0))
    for e in range(EXITS):
        block = logits[e].reshape(TOKENS, cols)
        log_total = turned_rows[:, e : e + 1]
        grad = (jnp.exp(block - log_total) - weight) * (loss_scale / TOKENS)
        dlogit[e * TOKENS : (e + 1) * TOKENS, :] = grad.astype(bf16)

    def fold_place(k):
        return lax.rem(y + lax.rem(k, 4), 4), lax.rem(xh + 1 - lax.div(k, 4), 2)

    def exchange(k):
        yk, xk = fold_place(k)
        return pltpu.make_async_remote_copy(
            src_ref=partial.at[yk, xk, :, :, :, 1 - c],
            dst_ref=swapped.at[yk, xk],
            send_sem=swap_send.at[k],
            recv_sem=swap_recv.at[k],
            device_id=partner,
            device_id_type=MESH,
        )

    def fold(k, _):
        yk, xk = fold_place(k)
        rows = head[head_rows(2 * yk + xk), :]
        part = lax.dot_general(
            dlogit[...], rows, (((1,), (1,)), ((), ())), preferred_element_type=f32
        )
        shape = (EXITS, 4, 2, 2, ROWS, width)
        partial[yk, xk] = part.astype(bf16).reshape(shape)
        exchange(k).start()
        return 0

    def add_swapped(k, _):
        yk, xk = fold_place(k)
        exchange(k).wait_recv()
        for e in range(EXITS):
            for low in range(2):
                mine = partial[yk, xk, e, :, low, c].astype(f32)
                theirs = swapped[yk, xk, e, :, low].astype(f32)
                partial[yk, xk, e, :, low, c] = (mine + theirs).astype(bf16)
        return 0

    def outer(k, _):
        part = lax.dot_general(
            rows_of(k), dlogit[...], (((0,), (0,)), ((), ())), preferred_element_type=f32
        )
        grad_head[head_rows(k), :] = part.astype(bf16)
        return 0

    terms = rows[EXITS : 2 * EXITS] + rows[:EXITS] * rows[2 * EXITS : 2 * EXITS + 1]
    mean = jnp.sum(terms, axis=1, keepdims=True) / TOKENS
    divergence[...] = jnp.broadcast_to(mean, (EXITS, 128))

    def add(e, axis, at, whole, part, arrived):
        dims = whole_dims(whole)

        def add_one(n):
            index = split_x({**pos, axis: at})
            found = []
            for d, size in reversed(dims):
                index[d] = lax.rem(n, size)
                found.insert(0, index[d])
                n = lax.div(n, size)
            ref = partial.at[
                index["y"], index["xh"], e, index["z"], index["xl"], c, :, columns_of(part)
            ]
            total = ref[...].astype(f32)
            for slot in arrived:
                total = total + slot[tuple(found)].astype(f32)
            ref[...] = total.astype(bf16)

        def step(n, _):
            for k in range(4):
                add_one(4 * n + k)
            return 0

        lax.fori_loop(0, 4 ** (len(whole) - 1), step, 0)

    def first_copies(e, axis, whole, slots):
        after, _, before = around(axis)
        up, far, down = (turned(pos[axis], k) for k in (1, 2, 3))
        return [
            copies.start(region(partial, e, {axis: far}, whole, 0), slots.at[0], after),
            copies.start(region(partial, e, {axis: far}, whole, 1), slots.at[1], before),
            copies.start(region(partial, e, {axis: up}, whole, 1), slots.at[3], after),
            copies.start(region(partial, e, {axis: down}, whole, 0), slots.at[4], before),
        ]

    def first_group(group):
        high = lax.rem(xh + 1 - group, 2)
        went = [[], [], []]
        if group == 0:
            after, _, before = around("x")
            for part, there in ((0, after), (1, before)):
                block = region(partial, 0, {"x": turned(x, 2)}, ("y", "z"), part)
                went[0].append(copies.start(block, first_0.at[part], there))
        side = xl if group == 0 else 1 - xl
        by = 3 + 2 * side
        block = partial.at[
            :, high, 0, :, 1 - xl, c, :, pl.ds(pl.multiple_of(side * half, 128), half)
        ]
        went[0].append(copies.start(block, first_0.at[4 - side], neighbour(pos, c, "x", by)))
        for e, axis, slots in ((1, "y", first_1), (2, "z", first_2)):
            after, _, before = around(axis)
            up, far, down = (turned(pos[axis], k) for k in (1, 2, 3))
            plan = ((far, 0, 0, after), (far, 1, 1, before), (up, 1, 3, after), (down, 0, 4, before))
            for at, part, slot, there in plan:
                place_z = slice(None) if axis == "y" else at
                place_y = at if axis == "y" else slice(None)
                block = partial.at[place_y, high, e, place_z, :, c, :, columns_of(part)]
                into = slots.at[slot, high] if axis == "y" else slots.at[slot, :, high]
                went[e].append(copies.start(block, into, there))
        return went

    def relay(e, axis, whole, slots, low, high):
        after, _, before = around(axis)
        up, down = turned(pos[axis], 1), turned(pos[axis], 3)
        for copy in low:
            copy.wait_recv()
        add(e, axis, up, whole, 0, [slots.at[0]])
        block = region(partial, e, {axis: up}, whole, 0)
        sent = [copies.start(block, slots.at[2], after)]
        for copy in high:
            copy.wait_recv()
        add(e, axis, down, whole, 1, [slots.at[1]])
        block = region(partial, e, {axis: down}, whole, 1)
        return sent + [copies.start(block, slots.at[5], before)]

    def last_sums(e, axis, whole, slots, waits):
        for copy in waits:
            copy.wait_recv()
        for part in range(2):
            add(e, axis, pos[axis], whole, part, [slots.at[2 + part], slots.at[4 + part]])

    first = (first_0, first_1, first_2)
    columns = []
    for e in range(EXITS):
        grad = dlogit[e * TOKENS : (e + 1) * TOKENS, :].astype(f32)
        columns.append(jnp.sum(grad * logits[e].reshape(TOKENS, cols), axis=1, keepdims=True))
    inner_vocab[v] = jnp.transpose(by_lane(columns, TOKENS))[:8]
    inner_copies = begin(copies, inner_vocab, v, vocab_peers(s, v))
    lax.fori_loop(0, 5, fold, 0)
    wait_for(inner_copies)
    inner_section[s] = slots_sum(inner_vocab, 16)
    inner_copies = begin(copies, inner_section, s, section_peers(s, v))
    lax.fori_loop(0, 4, add_swapped, 0)
    near_half = first_group(0)
    lax.fori_loop(5, 8, fold, 0)
    lax.fori_loop(4, 8, add_swapped, 0)
    own_half = first_group(1)
    lax.fori_loop(0, 5, outer, 0)
    waits = []
    for e in range(EXITS):
        one, two = near_half[e], own_half[e]
        if e == 0:
            low, high, rest = one[:1], one[1:2], one[2:] + two
        else:
            low, high, rest = [one[0], two[0]], [one[1], two[1]], one[2:] + two[2:]
        waits.append(rest + relay(e, ORDER[e][2], ORDER[e][:2], first[e], low, high))
    lax.fori_loop(5, 8, outer, 0)
    for e in range(EXITS):
        last_sums(e, ORDER[e][2], ORDER[e][:2], first[e], waits[e])
    wait_for(inner_copies)
    inner = slots_sum(inner_section, 8)
    inner_rows[...] = jnp.transpose(jnp.concatenate([inner, jnp.zeros((120, TOKENS), f32)], axis=0))
    second = (second_0, second_1, second_2)
    began = [first_copies(e, ORDER[e][1], ORDER[e][:1], second[e]) for e in range(EXITS)]
    waits = []
    for e in range(EXITS):
        low, high = began[e][:1], began[e][1:2]
        sent = relay(e, ORDER[e][1], ORDER[e][:1], second[e], low, high)
        waits.append(began[e][2:] + sent)
    for e in range(EXITS):
        last_sums(e, ORDER[e][1], ORDER[e][:1], second[e], waits[e])
    own_inner = inner_rows[pl.ds(pl.multiple_of(v * ROWS, ROWS), ROWS), :]
    removed = inverse[...] * inverse[...] * own_inner / (8 * width)
    went = []
    for e in range(EXITS):
        axis = ORDER[e][0]
        for k, there in enumerate(around(axis)):
            block = region(partial, e, {axis: turned(pos[axis], k + 1)}, (), None)
            went.append(copies.start(block, third.at[e, k], there))
    for e in range(EXITS):
        total = partial[y, xh, e, z, xl, c].astype(f32)
        for k in range(3):
            went[3 * e + k].wait_recv()
            total = total + third[e, k].astype(f32)
        scale = column_of(inverse[...], e)
        back = scale * (gain[e : e + 1, :] * total) - hidden[e].astype(f32) * column_of(removed, e)
        grad_hidden[e] = back.astype(bf16)
    copies.finish()
    for k in range(8):
        exchange(k).wait_send()


def body(exit_hidden, norm_gain, head_weight, teacher):
    width, cols = exit_hidden.shape[2], head_weight.shape[1]
    half = width // 2
    vmem = pl.BlockSpec(memory_space=pltpu.VMEM)
    hbm = pl.BlockSpec(memory_space=pltpu.HBM)
    dma = pltpu.SemaphoreType.DMA
    tile = (4, 2, EXITS, 4, 2, 2, ROWS, width)
    divergence, grad_hidden, grad_head = pl.pallas_call(
        kernel,
        out_shape=(
            jax.ShapeDtypeStruct((EXITS, 128), f32),
            jax.ShapeDtypeStruct(exit_hidden.shape, bf16),
            pltpu.VMEM(head_weight.shape, bf16),
        ),
        in_specs=[hbm] * 4,
        out_specs=(vmem,) * 3,
        scratch_shapes=[
            pltpu.VMEM(exit_hidden.shape, bf16),
            pltpu.VMEM(norm_gain.shape, f32),
            pltpu.VMEM(teacher.shape, f32),
            pltpu.VMEM(tile, bf16),
            pltpu.VMEM(head_weight.shape, bf16),
            pltpu.VMEM((EXITS, 4, 2, 2, ROWS, cols), f32),
            pltpu.VMEM((16, ROWS, cols), f32),
            pltpu.VMEM((EXITS * TOKENS, cols), bf16),
            pltpu.VMEM((ROWS, 128), f32),
            pltpu.VMEM(tile, bf16),
            pltpu.VMEM((4, 2, EXITS, 4, 2, ROWS, width), bf16),
        ]
        + [
            pltpu.VMEM((6, *(n for _, n in whole_dims(ORDER[e][:whole])), ROWS, half), bf16)
            for whole in (2, 1)
            for e in range(EXITS)
        ]
        + [
            pltpu.VMEM((EXITS, 3, ROWS, width), bf16),
            pltpu.VMEM((8, ROWS, 128), f32),
            pltpu.VMEM((16, 8, TOKENS), f32),
            pltpu.VMEM((8, 8, TOKENS), f32),
            pltpu.VMEM((8, *norm_gain.shape), f32),
            pltpu.VMEM((8, ROWS, 128), f32),
            pltpu.VMEM((16, 8, TOKENS), f32),
            pltpu.VMEM((8, 8, TOKENS), f32),
            pltpu.VMEM((TOKENS, 128), f32),
            dma((199,)),
            dma((199,)),
            dma((8,)),
            dma((8,)),
            dma((4,)),
        ],
        compiler_params=pltpu.CompilerParams(
            collective_id=0, has_side_effects=True, vmem_limit_bytes=53 * 2**20
        ),
        name="exits",
    )(exit_hidden, norm_gain, teacher, head_weight)
    return divergence[:, 0], grad_hidden, grad_head


def solution(mesh):
    return jax.shard_map(
        body,
        mesh=mesh,
        in_specs=(
            P(None, "vocab", "section"),
            P(None, "section"),
            P(None, ("section", "vocab")),
            P("vocab", "section"),
        ),
        out_specs=(P(), P(None, "vocab", "section"), P(None, ("section", "vocab"))),
        check_vma=False,
    )
```

```python
import functools

import jax
import jax.numpy as jnp
from jax import lax
from jax.experimental import pallas as pl
from jax.experimental.pallas import tpu as pltpu
from jax.sharding import PartitionSpec as P

MESH = pl.DeviceIdType.MESH
EXITS = 3
ROWS = 16
TOKENS = 256
epsilon = 1e-05
loss_scale = 1024.0
AXES = ("x", "y", "z")
ORDER = (("y", "z", "x"), ("z", "x", "y"), ("x", "y", "z"))
bf16 = jnp.bfloat16
f32 = jnp.float32


def chip(x, y, z, c):
    return (y * 2 + lax.div(x, 2), z * 4 + lax.rem(x, 2) * 2 + c)


def place():
    s, v = lax.axis_index("section"), lax.axis_index("vocab")
    x = lax.rem(s, 2) * 2 + lax.rem(lax.div(v, 2), 2)
    return s, v, dict(x=x, y=lax.div(s, 2), z=lax.div(v, 4)), lax.rem(v, 2)


def turned(k, by):
    return lax.rem(k + by, 4)


class Copies:
    def __init__(self, send_sem, recv_sem):
        self.send_sem, self.recv_sem, self.made, self.left = send_sem, recv_sem, [], 0

    def start(self, src, dst, device):
        n = len(self.made)
        copy = pltpu.make_async_remote_copy(
            src_ref=src,
            dst_ref=dst,
            send_sem=self.send_sem.at[n],
            recv_sem=self.recv_sem.at[n],
            device_id=device,
            device_id_type=MESH,
        )
        copy.start()
        self.made.append(copy)
        return copy

    def finish(self):
        for copy in self.made[self.left :]:
            copy.wait_send()
        self.left = len(self.made)


def neighbour(pos, c, axis, by):
    there = dict(pos)
    there[axis] = turned(pos[axis], by)
    return chip(**there, c=c)


def greet(devices):
    barrier = pltpu.get_barrier_semaphore()
    for device in devices:
        pl.semaphore_signal(barrier, inc=1, device_id=device, device_id_type=MESH)
    return lambda: pl.semaphore_wait(barrier, len(devices))


def section_peers(s, v):
    return [(lax.rem(s + k, 8), v) for k in range(1, 8)]


def vocab_peers(s, v):
    return [(s, lax.rem(v + k, 16)) for k in range(1, 16)]


DIMS = (("y", 4), ("xh", 2), ("z", 4), ("xl", 2))


def split_x(pos):
    return {
        "y": pos["y"],
        "xh": lax.div(pos["x"], 2),
        "z": pos["z"],
        "xl": lax.rem(pos["x"], 2),
    }


def whole_dims(whole):
    return [(d, n) for d, n in DIMS if d[0] in whole]


def begin(copies, slots, me, peers):
    return [copies.start(slots.at[me], slots.at[me], peer) for peer in peers]


def wait_for(sent):
    for copy in sent:
        copy.wait_recv()


def to_all(copies, slots, me, peers):
    wait_for(begin(copies, slots, me, peers))


def by_lane(columns, rows):
    lane = lax.broadcasted_iota(jnp.int32, (rows, 128), 1)
    tile = jnp.zeros((rows, 128), f32)
    for k, column in enumerate(columns):
        tile = jnp.where(lane == k, column, tile)
    return tile


def column_of(tile, k):
    lane = lax.broadcasted_iota(jnp.int32, tile.shape, 1)
    return jnp.sum(jnp.where(lane == k, tile, 0.0), axis=1, keepdims=True)


def slots_sum(slots, count):
    total = slots[0]
    for k in range(1, count):
        total = total + slots[k]
    return total


def merged(slots, count):
    top = slots[0]
    for k in range(1, count):
        top = jnp.maximum(top, slots[k])
    exps = jnp.zeros(top.shape, f32)
    for k in range(count):
        exps = exps + jnp.exp(slots[k] - top)
    return top + jnp.log(exps)


def kernel(
    hidden_hbm, gain_hbm, teacher_hbm, head_hbm, divergence, grad_hidden, grad_head,
    hidden, gain, teacher, full, head, logits, target, dlogit, inverse, partial, swapped,
    first_0, first_1, first_2, second_0, second_1, second_2, third,
    square_slots, vocab_slots, section_slots, gain_slots, inverse_slots, inner_vocab, inner_section,
    inner_rows,
    send_sem, recv_sem, swap_send, swap_recv, local_sem,
):
    width, cols = hidden.shape[2], head.shape[1]
    half = width // 2
    s, v, pos, c = place()
    x, y, z = pos["x"], pos["y"], pos["z"]
    xh, xl = lax.div(x, 2), lax.rem(x, 2)
    partner = chip(**pos, c=1 - c)
    copies = Copies(send_sem, recv_sem)
    same_core = [(s, lax.rem(v + k, 16)) for k in range(2, 16, 2)]
    beyond = neighbour(pos, c, "x", 3 + 2 * xl)
    ready = greet([partner, beyond] + section_peers(s, v) + same_core)
    loads = [
        pltpu.make_async_copy(src, dst, local_sem.at[k])
        for k, (src, dst) in enumerate(
            ((hidden_hbm, hidden), (gain_hbm, gain), (head_hbm, head), (teacher_hbm, teacher))
        )
    ]
    for load in loads:
        load.start()
    loads[0].wait()
    squares = [
        jnp.sum(jnp.square(hidden[e].astype(f32)), axis=1, keepdims=True) for e in range(EXITS)
    ]
    square_slots[s] = by_lane(squares, ROWS)
    for e in range(EXITS):
        full[y, xh, e, z, xl, c] = hidden[e]
    loads[1].wait()
    gain_slots[s] = gain[...]
    ready()
    square_copies = begin(copies, square_slots, s, section_peers(s, v))

    def columns_of(part):
        return slice(None) if part is None else slice(part * half, (part + 1) * half)

    def region(ref, e, over, whole, part):
        at = split_x({**pos, **over})
        for d, _ in whole_dims(whole):
            at[d] = slice(None)
        return ref.at[at["y"], at["xh"], e, at["z"], at["xl"], c, :, columns_of(part)]

    def around(axis):
        return [neighbour(pos, c, axis, by) for by in (1, 2, 3)]

    def swap(ref):
        return copies.start(ref, ref, partner)

    def rows_of(k):
        return full[lax.div(k, 2), lax.rem(k, 2)].reshape(EXITS * TOKENS, width)

    def head_rows(k):
        return pl.ds(pl.multiple_of(k * width, 128), width)

    def across_x(by):
        there = turned(x, by)
        high, low = lax.div(there, 2), lax.rem(there, 2)

        def step(k, _):
            tokens = full[k, high, 0, :, low].reshape(TOKENS // 2, width)
            part = jnp.dot(tokens, head[head_rows(2 * k + high), :], preferred_element_type=f32)
            logits[0, :, low] += part.reshape(4, 2, ROWS, cols)
            return 0

        lax.fori_loop(0, 4, step, 0)

    def across_y(by):
        there = turned(y, by)

        def step(k, _):
            tokens = full[there, k, 1].reshape(TOKENS, width)
            part = jnp.dot(tokens, head[head_rows(2 * there + k), :], preferred_element_type=f32)
            logits[1] += part.reshape(4, 2, 2, ROWS, cols)
            return 0

        lax.fori_loop(0, 2, step, 0)

    def last_exit(k, _):
        yk, xk = lax.div(k, 2), lax.rem(k, 2)
        places = [z, turned(z, 1), turned(z, 3)]
        tokens = [full[yk, xk, 2, at].reshape(TOKENS // 4, width) for at in places]
        rows = head[head_rows(k), :]
        part = jnp.dot(jnp.concatenate(tokens, axis=0), rows, preferred_element_type=f32)
        part = part.reshape(3, 2, 2, ROWS, cols)
        for n, at in enumerate(places):
            logits[2, at] += part[n]
        return 0

    def far_blocks(yk, xk, with_y, with_x):
        far_x, far_z = turned(x, 2), turned(z, 2)
        low = lax.rem(far_x, 2)
        tokens = [full[yk, xk, 2, far_z].reshape(TOKENS // 4, width)]
        if with_x:
            tokens.append(full[yk, xk, 0, :, low].reshape(TOKENS // 2, width))
        if with_y:
            tokens.append(full[yk, xk, 1].reshape(TOKENS, width))
        tokens = jnp.concatenate(tokens, axis=0) if len(tokens) > 1 else tokens[0]
        part = jnp.dot(tokens, head[head_rows(2 * yk + xk), :], preferred_element_type=f32)
        at = TOKENS // 4
        logits[2, far_z] += part[:at].reshape(2, 2, ROWS, cols)
        if with_x:
            logits[0, :, low] += part[at : at + TOKENS // 2].reshape(4, 2, ROWS, cols)
            at += TOKENS // 2
        if with_y:
            logits[1] += part[at:].reshape(4, 2, 2, ROWS, cols)

    def far_step(k, _):
        yk = turned(y, 3 + k)
        far_blocks(yk, 1 - xh, False, True)
        far_blocks(yk, xh, False, False)
        return 0

    logits[...] = jnp.zeros(logits.shape, f32)

    sent = []
    for e in range(EXITS):
        mine = region(full, e, {}, (), None)
        sent += [copies.start(mine, mine, there) for there in around(ORDER[e][0])]
    gain_copies = [copies.start(gain, gain_slots.at[s], peer) for peer in section_peers(s, v)]
    wait_for(sent)

    def normalise(block, scale, gains):
        block[...] = (block[...].astype(f32) * scale * gains).astype(bf16)

    def normalise_step(k, _):
        for n in range(4):
            high, low = divmod(n, 2)
            normalise(
                full.at[k, xh, 0, n, xl, c],
                inverse_slots[2 * n + xl][:, 0:1],
                gain_slots[2 * k + xh][0:1, :],
            )
            normalise(
                full.at[y, high, 1, k, low, c],
                inverse_slots[2 * k + low][:, 1:2],
                gain_slots[2 * y + high][1:2, :],
            )
            normalise(
                full.at[k, high, 2, z, low, c],
                inverse_slots[2 * z + low][:, 2:3],
                gain_slots[2 * k + high][2:3, :],
            )
        return 0

    for turn in (1, 2):
        last = turn == 2
        pieces = []
        if last:
            wait_for(gain_copies + inverse_copies)
            copies.finish()
            lax.fori_loop(0, 4, normalise_step, 0)
        for e in range(EXITS):
            axis, whole = ORDER[e][turn], ORDER[e][:turn]
            after, _, before = around(axis)
            low, high = region(full, e, {}, whole, 0), region(full, e, {}, whole, 1)
            up_low = copies.start(low, low, after)
            down_high = copies.start(high, high, before)
            up_high = copies.start(high, high, after)
            down_low = copies.start(low, low, before)
            pieces.append((up_low, down_high, up_high, down_low))
        if last:
            own_swaps = [swap(region(full, e, {}, ORDER[e][:2], None)) for e in range(EXITS)]
            near_swaps = [[], [], []]
            far_swaps = []
            loads[2].wait()
            for e in range(2):
                own_swaps[e].wait_recv()
                (across_x, across_y)[e](0)
        else:
            wait_for(square_copies)
            inverse[...] = lax.rsqrt(slots_sum(square_slots, 8) / (8 * width) + epsilon)
            inverse_slots[lax.div(v, 2)] = inverse[...]
            inverse_copies = begin(copies, inverse_slots, lax.div(v, 2), same_core)
        relays = []
        for e in range(EXITS):
            axis, whole = ORDER[e][turn], ORDER[e][:turn]
            after, _, before = around(axis)
            up_low, down_high, _, _ = pieces[e]
            up_low.wait_recv()
            block = region(full, e, {axis: turned(pos[axis], 3)}, whole, 0)
            up = copies.start(block, block, after)
            if last:
                near_swaps[e].append(swap(block))
            down_high.wait_recv()
            block = region(full, e, {axis: turned(pos[axis], 1)}, whole, 1)
            down = copies.start(block, block, before)
            if last:
                near_swaps[e].append(swap(block))
            relays.append((up, down))
        for e in range(EXITS):
            axis, whole = ORDER[e][turn], ORDER[e][:turn]
            pieces[e][2].wait_recv()
            if last:
                near_swaps[e].append(swap(region(full, e, {axis: turned(pos[axis], 3)}, whole, 1)))
            pieces[e][3].wait_recv()
            if last:
                near_swaps[e].append(swap(region(full, e, {axis: turned(pos[axis], 1)}, whole, 0)))
        if last:
            loads[3].wait()
            lent = [
                copies.start(
                    teacher.at[:, pl.ds(pl.multiple_of(peer[1] * cols, 128), cols)],
                    target.at[v],
                    peer,
                )
                for peer in vocab_peers(s, v)
            ]
            target[v] = teacher[:, pl.ds(pl.multiple_of(v * cols, 128), cols)]
            for e in range(2):
                for copy in near_swaps[e]:
                    copy.wait_recv()
                (across_x, across_y)[e](1)
                (across_x, across_y)[e](3)
            wait_for([own_swaps[2]] + near_swaps[2])
            lax.fori_loop(0, 4, last_exit, 0)
        for e in range(EXITS):
            axis, whole = ORDER[e][turn], ORDER[e][:turn]
            for k in range(2):
                relays[e][k].wait_recv()
                if last:
                    block = region(full, e, {axis: turned(pos[axis], 2)}, whole, k)
                    far_swaps.append(swap(block))
    lax.fori_loop(4, 8, last_exit, 0)
    wait_for(far_swaps)
    far_blocks(turned(y, 2), 1 - xh, True, True)
    far_blocks(turned(y, 2), xh, True, False)
    lax.fori_loop(0, 3, far_step, 0)

    columns = []
    for e in range(EXITS):
        block = logits[e].reshape(TOKENS, cols)
        top = jnp.max(block, axis=1, keepdims=True)
        columns.append(top + jnp.log(jnp.sum(jnp.exp(block - top), axis=1, keepdims=True)))
    vocab_slots[v] = jnp.transpose(by_lane(columns, TOKENS))[:8]
    total_copies = begin(copies, vocab_slots, v, vocab_peers(s, v))
    wait_for(lent)
    stored = target[...].reshape(TOKENS, cols)
    weight = jnp.exp(stored)
    teacher_columns = []
    for e in range(EXITS):
        block = logits[e].reshape(TOKENS, cols)
        teacher_columns.append(jnp.sum(weight * (stored - block), axis=1, keepdims=True))
    teacher_columns.append(jnp.sum(weight, axis=1, keepdims=True))
    target[...] = weight.reshape(16, ROWS, cols)
    wait_for(total_copies)
    section_slots[s] = merged(vocab_slots, 16)
    to_all(copies, section_slots, s, section_peers(s, v))
    rows = merged(section_slots, 8)
    turned_rows = jnp.transpose(jnp.concatenate([rows, jnp.zeros((120, TOKENS), f32)], axis=0))
    for e in range(EXITS):
        block = logits[e].reshape(TOKENS, cols)
        log_total = turned_rows[:, e : e + 1]
        weight = target[...].reshape(TOKENS, cols)
        grad = (jnp.exp(block - log_total) - weight) * (loss_scale / TOKENS)
        dlogit[e * TOKENS : (e + 1) * TOKENS, :] = grad.astype(bf16)

    def fold_place(k):
        return lax.rem(y + lax.rem(k, 4), 4), lax.rem(xh + 1 - lax.div(k, 4), 2)

    def exchange(k):
        yk, xk = fold_place(k)
        return pltpu.make_async_remote_copy(
            src_ref=partial.at[yk, xk, :, :, :, 1 - c],
            dst_ref=swapped.at[yk, xk],
            send_sem=swap_send.at[k],
            recv_sem=swap_recv.at[k],
            device_id=partner,
            device_id_type=MESH,
        )

    def fold(k, _):
        yk, xk = fold_place(k)
        rows = head[head_rows(2 * yk + xk), :]
        part = lax.dot_general(
            dlogit[...], rows, (((1,), (1,)), ((), ())), preferred_element_type=f32
        )
        shape = (EXITS, 4, 2, 2, ROWS, width)
        partial[yk, xk] = part.astype(bf16).reshape(shape)
        exchange(k).start()
        return 0

    def add_swapped(k, _):
        yk, xk = fold_place(k)
        exchange(k).wait_recv()
        for e in range(EXITS):
            for low in range(2):
                mine = partial[yk, xk, e, :, low, c].astype(f32)
                theirs = swapped[yk, xk, e, :, low].astype(f32)
                partial[yk, xk, e, :, low, c] = (mine + theirs).astype(bf16)
        return 0

    def outer(k, _):
        part = lax.dot_general(
            rows_of(k), dlogit[...], (((0,), (0,)), ((), ())), preferred_element_type=f32
        )
        grad_head[head_rows(k), :] = part.astype(bf16)
        return 0

    def add(e, axis, at, whole, part, arrived):
        dims = whole_dims(whole)

        def add_one(n):
            index = split_x({**pos, axis: at})
            found = []
            for d, size in reversed(dims):
                index[d] = lax.rem(n, size)
                found.insert(0, index[d])
                n = lax.div(n, size)
            ref = partial.at[
                index["y"], index["xh"], e, index["z"], index["xl"], c, :, columns_of(part)
            ]
            total = ref[...].astype(f32)
            for slot in arrived:
                total = total + slot[tuple(found)].astype(f32)
            ref[...] = total.astype(bf16)

        def step(n, _):
            for k in range(4):
                add_one(4 * n + k)
            return 0

        lax.fori_loop(0, 4 ** (len(whole) - 1), step, 0)

    def first_copies(e, axis, whole, slots):
        after, _, before = around(axis)
        up, far, down = (turned(pos[axis], k) for k in (1, 2, 3))
        return [
            copies.start(region(partial, e, {axis: far}, whole, 0), slots.at[0], after),
            copies.start(region(partial, e, {axis: far}, whole, 1), slots.at[1], before),
            copies.start(region(partial, e, {axis: up}, whole, 1), slots.at[3], after),
            copies.start(region(partial, e, {axis: down}, whole, 0), slots.at[4], before),
        ]

    def first_group(group):
        high = lax.rem(xh + 1 - group, 2)
        went = [[], [], []]
        if group == 0:
            after, _, before = around("x")
            for part, there in ((0, after), (1, before)):
                block = region(partial, 0, {"x": turned(x, 2)}, ("y", "z"), part)
                went[0].append(copies.start(block, first_0.at[part], there))
        side = xl if group == 0 else 1 - xl
        by = 3 + 2 * side
        block = partial.at[
            :, high, 0, :, 1 - xl, c, :, pl.ds(pl.multiple_of(side * half, 128), half)
        ]
        went[0].append(copies.start(block, first_0.at[4 - side], neighbour(pos, c, "x", by)))
        for e, axis, slots in ((1, "y", first_1), (2, "z", first_2)):
            after, _, before = around(axis)
            up, far, down = (turned(pos[axis], k) for k in (1, 2, 3))
            plan = ((far, 0, 0, after), (far, 1, 1, before), (up, 1, 3, after), (down, 0, 4, before))
            for at, part, slot, there in plan:
                place_z = slice(None) if axis == "y" else at
                place_y = at if axis == "y" else slice(None)
                block = partial.at[place_y, high, e, place_z, :, c, :, columns_of(part)]
                into = slots.at[slot, high] if axis == "y" else slots.at[slot, :, high]
                went[e].append(copies.start(block, into, there))
        return went

    def relay(e, axis, whole, slots, low, high):
        after, _, before = around(axis)
        up, down = turned(pos[axis], 1), turned(pos[axis], 3)
        for copy in low:
            copy.wait_recv()
        add(e, axis, up, whole, 0, [slots.at[0]])
        block = region(partial, e, {axis: up}, whole, 0)
        sent = [copies.start(block, slots.at[2], after)]
        for copy in high:
            copy.wait_recv()
        add(e, axis, down, whole, 1, [slots.at[1]])
        block = region(partial, e, {axis: down}, whole, 1)
        return sent + [copies.start(block, slots.at[5], before)]

    def last_sums(e, axis, whole, slots, waits):
        for copy in waits:
            copy.wait_recv()
        for part in range(2):
            add(e, axis, pos[axis], whole, part, [slots.at[2 + part], slots.at[4 + part]])

    first = (first_0, first_1, first_2)
    columns = []
    for e in range(EXITS):
        grad = dlogit[e * TOKENS : (e + 1) * TOKENS, :].astype(f32)
        columns.append(jnp.sum(grad * logits[e].reshape(TOKENS, cols), axis=1, keepdims=True))
    inner_vocab[v] = jnp.transpose(by_lane(columns + teacher_columns, TOKENS))[:8]
    inner_copies = begin(copies, inner_vocab, v, vocab_peers(s, v))
    lax.fori_loop(0, 5, fold, 0)
    wait_for(inner_copies)
    inner_section[s] = slots_sum(inner_vocab, 16)
    inner_copies = begin(copies, inner_section, s, section_peers(s, v))
    lax.fori_loop(0, 4, add_swapped, 0)
    near_half = first_group(0)
    lax.fori_loop(5, 8, fold, 0)
    lax.fori_loop(4, 8, add_swapped, 0)
    own_half = first_group(1)
    lax.fori_loop(0, 5, outer, 0)
    waits = []
    for e in range(EXITS):
        one, two = near_half[e], own_half[e]
        if e == 0:
            low, high, rest = one[:1], one[1:2], one[2:] + two
        else:
            low, high, rest = [one[0], two[0]], [one[1], two[1]], one[2:] + two[2:]
        waits.append(rest + relay(e, ORDER[e][2], ORDER[e][:2], first[e], low, high))
    lax.fori_loop(5, 8, outer, 0)
    for e in range(EXITS):
        last_sums(e, ORDER[e][2], ORDER[e][:2], first[e], waits[e])
    wait_for(inner_copies)
    inner = slots_sum(inner_section, 8)
    terms = inner[EXITS : 2 * EXITS] + rows[:EXITS] * inner[2 * EXITS : 2 * EXITS + 1]
    for e in range(EXITS):
        divergence[e] = jnp.sum(terms[e : e + 1, :]) / TOKENS
    inner_rows[...] = jnp.transpose(jnp.concatenate([inner, jnp.zeros((120, TOKENS), f32)], axis=0))
    second = (second_0, second_1, second_2)
    began = [first_copies(e, ORDER[e][1], ORDER[e][:1], second[e]) for e in range(EXITS)]
    waits = []
    for e in range(EXITS):
        low, high = began[e][:1], began[e][1:2]
        sent = relay(e, ORDER[e][1], ORDER[e][:1], second[e], low, high)
        waits.append(began[e][2:] + sent)
    for e in range(EXITS):
        last_sums(e, ORDER[e][1], ORDER[e][:1], second[e], waits[e])
    own_inner = inner_rows[pl.ds(pl.multiple_of(v * ROWS, ROWS), ROWS), :]
    removed = inverse[...] * inverse[...] * own_inner / (8 * width)
    went = []
    for e in range(EXITS):
        axis = ORDER[e][0]
        for k, there in enumerate(around(axis)):
            block = region(partial, e, {axis: turned(pos[axis], k + 1)}, (), None)
            went.append(copies.start(block, third.at[e, k], there))
    for e in range(EXITS):
        total = partial[y, xh, e, z, xl, c].astype(f32)
        for k in range(3):
            went[3 * e + k].wait_recv()
            total = total + third[e, k].astype(f32)
        scale = column_of(inverse[...], e)
        back = scale * (gain[e : e + 1, :] * total) - hidden[e].astype(f32) * column_of(removed, e)
        grad_hidden[e] = back.astype(bf16)
    copies.finish()
    for k in range(8):
        exchange(k).wait_send()


def body(exit_hidden, norm_gain, head_weight, teacher):
    width, cols = exit_hidden.shape[2], head_weight.shape[1]
    half = width // 2
    vmem = pl.BlockSpec(memory_space=pltpu.VMEM)
    hbm = pl.BlockSpec(memory_space=pltpu.HBM)
    dma = pltpu.SemaphoreType.DMA
    tile = (4, 2, EXITS, 4, 2, 2, ROWS, width)
    divergence, grad_hidden, grad_head = pl.pallas_call(
        kernel,
        out_shape=(
            jax.ShapeDtypeStruct((EXITS,), f32),
            jax.ShapeDtypeStruct(exit_hidden.shape, bf16),
            pltpu.VMEM(head_weight.shape, bf16),
        ),
        in_specs=[hbm] * 4,
        out_specs=(pl.BlockSpec(memory_space=pltpu.SMEM), vmem, vmem),
        scratch_shapes=[
            pltpu.VMEM(exit_hidden.shape, bf16),
            pltpu.VMEM(norm_gain.shape, f32),
            pltpu.VMEM(teacher.shape, f32),
            pltpu.VMEM(tile, bf16),
            pltpu.VMEM(head_weight.shape, bf16),
            pltpu.VMEM((EXITS, 4, 2, 2, ROWS, cols), f32),
            pltpu.VMEM((16, ROWS, cols), f32),
            pltpu.VMEM((EXITS * TOKENS, cols), bf16),
            pltpu.VMEM((ROWS, 128), f32),
            pltpu.VMEM(tile, bf16),
            pltpu.VMEM((4, 2, EXITS, 4, 2, ROWS, width), bf16),
        ]
        + [
            pltpu.VMEM((6, *(n for _, n in whole_dims(ORDER[e][:whole])), ROWS, half), bf16)
            for whole in (2, 1)
            for e in range(EXITS)
        ]
        + [
            pltpu.VMEM((EXITS, 3, ROWS, width), bf16),
            pltpu.VMEM((8, ROWS, 128), f32),
            pltpu.VMEM((16, 8, TOKENS), f32),
            pltpu.VMEM((8, 8, TOKENS), f32),
            pltpu.VMEM((8, *norm_gain.shape), f32),
            pltpu.VMEM((8, ROWS, 128), f32),
            pltpu.VMEM((16, 8, TOKENS), f32),
            pltpu.VMEM((8, 8, TOKENS), f32),
            pltpu.VMEM((TOKENS, 128), f32),
            dma((199,)),
            dma((199,)),
            dma((8,)),
            dma((8,)),
            dma((4,)),
        ],
        compiler_params=pltpu.CompilerParams(
            collective_id=0, has_side_effects=True, vmem_limit_bytes=53 * 2**20
        ),
        name="exits",
    )(exit_hidden, norm_gain, teacher, head_weight)
    return divergence, grad_hidden, grad_head


def solution(mesh):
    return jax.shard_map(
        body,
        mesh=mesh,
        in_specs=(
            P(None, "vocab", "section"),
            P(None, "section"),
            P(None, ("section", "vocab")),
            P("vocab", "section"),
        ),
        out_specs=(P(), P(None, "vocab", "section"), P(None, ("section", "vocab"))),
        check_vma=False,
    )
```
